128 devices in a mesh: grp: 4 (over z_lo, core), blk: 32 (over x, z_hi, y).
Axes of the slice: x: 4, y: 4, z: 4 (z_hi: 2, z_lo: 2; z = z_hi * 2 + z_lo), core: 2. Of those that a mesh axis runs over, the one named last changes fastest.
Arguments:
- residual: float32 [3, 64, 128, 512], P(None, 'blk', None, 'grp'), may hold values from -8 to 8
- face_mask: int32 [3, 64, 128, 512], P(None, 'blk', None, 'grp'), may hold values 0 or 1
- conductivity: float32 [4, 64, 128, 512], P('grp', 'blk'), may hold values from 0.5 to 4
- stencil: float32 [4, 27, 3, 3], replicated, may hold values from -1.5 to 1.5, as said below
Outputs:
- correction: float32 [3, 64, 128, 512], P(None, 'blk', None, 'grp')
The draws below stay inside these ranges and needn't reach their ends.
Inputs may be any that keep to these rules, and one draw needn't show every extreme that they name: In each space's stencil the diagonal of the block at offset 0 exceeds the sum of magnitudes of all other entries of its row.
All inputs are finite; a program needn't handle non-finite values. No bound on the sum of `face_mask` on one device may be relied on, other than what follows from the above.
Results may differ from the reference program's by a relative error of at most 0.0001.
Values sent between devices are 32-bit elements; how exact they have to be, the bound alone decides.
No kernel may reach another device: no remote copies, remote signals or barrier semaphores. Data moves between devices by JAX's collectives and lax.ppermute only.
A program may use at most 192 MiB of HBM per device.

```python
import math
import jax
import jax.numpy as jnp

NY = 128
NZ = 512
NX = 64


def draw_stencil(key, part):
    key_off = jax.random.fold_in(key, 11)
    key_diag = jax.random.fold_in(key, 12)
    key_cross = jax.random.fold_in(key, 13)
    offdiag = 0.01 * jax.random.normal(key_off, (4, 27, 3, 3), jnp.float32)
    diagonal = 1.0 + 0.5 * jax.random.uniform(key_diag, (4, 3), jnp.float32)
    cross = jnp.clip(0.1 * jax.random.normal(key_cross, (4, 3, 3), jnp.float32), -0.1, 0.1)
    identity = jnp.eye(3, dtype=jnp.float32)
    offdiag = jnp.clip(offdiag, -0.017, 0.017)
    centre = diagonal[:, :, None] * identity + cross * (1.0 - identity)
    return offdiag.at[:, 13].set(centre)


def place_ends(entries, rng, smallest, high):
    index_at = [jax.random.randint(jax.random.fold_in(rng, axis), (), 0, length) for axis, length in enumerate(entries.shape)]
    main_axis = entries.shape.index(max(entries.shape))
    beside = index_at[:main_axis] + [(index_at[main_axis] + 1) % entries.shape[main_axis]] + index_at[main_axis + 1:]
    return entries.at[tuple(index_at)].set(smallest).at[tuple(beside)].set(high)


def steps_of(key, dims, shards, smallest, largest):
    level, own = 1.0, jax.random.fold_in(key, 6)
    for position, parts in shards:
        draws = jnp.exp(jax.random.uniform(jax.random.fold_in(own, position), (parts,), jnp.float32, smallest / len(shards), largest / len(shards)))
        level = level * jnp.repeat(draws, dims[position] // parts).reshape([-1 if axis == position else 1 for axis in range(len(dims))])
    return level


def normal_values(stream_key, extent, scale, reach, shards=(), held_as=jnp.bfloat16):
    gain = steps_of(stream_key, extent, shards, -0.22, 0.18) if shards else 1.0
    array = jax.random.normal(stream_key, extent, jnp.float32) * scale * gain
    return jnp.minimum(jnp.maximum(array, -reach), reach).astype(held_as)


def setup_inputs(seed: int = 0) -> dict:
    key_of = jax.random.split(jax.random.key(seed), 5)
    return {
        "residual": normal_values(key_of[0], (3, NX, NY, NZ), 1.0, 8.0, ((1, 32), (3, 4)), jnp.float32),
        "face_mask": place_ends((jax.random.randint(key_of[1], (3, NX, NY, NZ), 0, 8) < 7).astype(jnp.int32), jax.random.fold_in(key_of[1], 1), 0, 1),
        "conductivity": jnp.clip(jnp.exp(math.log(4.0) - 2.0794415 * jax.random.uniform(key_of[2], (4, NX, NY, NZ), jnp.float32) ** steps_of(key_of[2], (4, NX, NY, NZ), ((0, 4), (1, 32)), -0.2, 0.2)), 0.5, 4.0),
        "stencil": draw_stencil(jax.random.fold_in(key_of[4], 71), 0),
    }


OMEGA = 0.8


def place_of(shift_x, shift_y, shift_z):
    return 9 * (shift_x + 1) + 3 * (shift_y + 1) + (shift_z + 1)


def blank_tables():
    return [[[[0.0, 0.0, 0.0] for row_one in range(3)] for place in range(27)] for space in range(4)]


def restriction_tables():
    forward = blank_tables()
    centre = place_of(0, 0, 0)
    for comp in range(3):
        forward[0][centre][comp][comp] = 1.0
        others = [axis_one for axis_one in range(3) if axis_one != comp]
        for first_off in (0, -1):
            for second_off in (0, -1):
                vector = [0, 0, 0]
                vector[others[0]] = first_off
                vector[others[1]] = second_off
                forward[1][place_of(*vector)][comp][comp] += 0.25
        along_p = (comp + 1) % 3
        along_q = (comp + 2) % 3
        forward[2][centre][comp][along_q] += 1.0
        forward[2][centre][comp][along_p] -= 1.0
        vector = [0, 0, 0]
        vector[along_p] = -1
        forward[2][place_of(*vector)][comp][along_q] -= 1.0
        vector = [0, 0, 0]
        vector[along_q] = -1
        forward[2][place_of(*vector)][comp][along_p] += 1.0
    for comp in range(3):
        for shift_x in (-1, 0, 1):
            for shift_y in (-1, 0, 1):
                for shift_z in (-1, 0, 1):
                    source = list(forward[2][place_of(shift_x, shift_y, shift_z)][comp])
                    if abs(source[0]) + abs(source[1]) + abs(source[2]) == 0:
                        continue
                    vector = [shift_x, shift_y, shift_z]
                    vector[comp] += 1
                    for column in range(3):
                        forward[3][place_of(shift_x, shift_y, shift_z)][comp][column] += 0.5 * source[column]
                        forward[3][place_of(*vector)][comp][column] += 0.5 * source[column]
    backward = blank_tables()
    for space in range(4):
        for shift_x in (-1, 0, 1):
            for shift_y in (-1, 0, 1):
                for shift_z in (-1, 0, 1):
                    for row_one in range(3):
                        for column in range(3):
                            backward[space][place_of(-shift_x, -shift_y, -shift_z)][row_one][column] = forward[space][place_of(shift_x, shift_y, shift_z)][column][row_one]
    return forward, backward


def stencil_apply(table, field):
    rows_x = field.shape[1] - 2
    rows_y = field.shape[2]
    rows_z = field.shape[3]
    padded = jnp.pad(field, ((0, 0), (0, 0), (1, 1), (1, 1)))
    total = jnp.zeros((3, rows_x, rows_y, rows_z), jnp.float32)
    for shift_x in (-1, 0, 1):
        for shift_y in (-1, 0, 1):
            for shift_z in (-1, 0, 1):
                piece = padded[:, 1 + shift_x:1 + shift_x + rows_x, 1 + shift_y:1 + shift_y + rows_y, 1 + shift_z:1 + shift_z + rows_z]
                block = table[place_of(shift_x, shift_y, shift_z)]
                total = total + (block[:, :, None, None, None] * piece[None]).sum(1)
    return total


def pad_first(field):
    return jnp.pad(field, ((0, 0), (1, 1), (0, 0), (0, 0)))


def reference(residual, face_mask, conductivity, stencil):
    mask_float = face_mask.astype(jnp.float32)
    masked = residual * mask_float
    forward, backward = restriction_tables()
    fwd_all = jnp.asarray(forward, jnp.float32)
    bwd_all = jnp.asarray(backward, jnp.float32)
    total = jnp.zeros(residual.shape, jnp.float32)
    for group in range(4):
        restricted = stencil_apply(fwd_all[group], pad_first(masked))
        centre = jnp.diagonal(stencil[group, 13])
        coeff = conductivity[group][None]
        scale = OMEGA / (coeff * centre[:, None, None, None])
        first = restricted * scale
        applied = coeff * stencil_apply(stencil[group], pad_first(first))
        second = first + (restricted - applied) * scale
        total = total + stencil_apply(bwd_all[group], pad_first(second))
    return total * mask_float
```

```python
import jax
import jax.numpy as jnp
from jax import lax
from jax.experimental import pallas as pl
from jax.experimental.pallas import tpu as pltpu
from jax.sharding import PartitionSpec as P

OMEGA = 0.8
F32 = jnp.float32
N = 128
INV = 136
ZLOW = 2 * INV
ZHIGH = ZLOW + 18
CHUNK = 312
SIDE = 4 * INV
MESSAGE = SIDE + 5 * 8
MROWS = 152
HROWS = 144
WROWS = 136
PARTS = ((0, 1), (1, 1), (2, 1), (1, 0), (2, 0))


def vmem():
    return pl.BlockSpec(memory_space=pltpu.VMEM)


def smem():
    return pl.BlockSpec(memory_space=pltpu.SMEM)


def call(kernel, name, out_shapes, in_specs, scratch=()):
    return pl.pallas_call(
        kernel,
        name=name,
        out_shape=[jax.ShapeDtypeStruct(shape, F32) for shape in out_shapes],
        in_specs=in_specs,
        out_specs=[vmem() for _ in out_shapes],
        scratch_shapes=list(scratch),
        compiler_params=pltpu.CompilerParams(vmem_limit_bytes=50 << 20),
    )


def from_below(v):
    lane = lax.broadcasted_iota(jnp.int32, v.shape, 1)
    return jnp.where(lane == 0, 0.0, pltpu.roll(v, 1, 1))


def from_above(v):
    lane = lax.broadcasted_iota(jnp.int32, v.shape, 1)
    return jnp.where(lane == N - 1, 0.0, pltpu.roll(v, N - 1, 1))


def prepare(res, mask, cond, own, to_high, to_low, chunks):
    for comp in range(3):
        for layer in range(2):
            v = (res[comp, layer] * mask[comp, layer].astype(F32)).T
            own[comp, layer] = v
            row = (comp * 2 + layer) * 3
            for q in range(4):
                chunks[q, ZLOW + row : ZLOW + row + 3] = v[0:3]
                chunks[q, ZHIGH + row : ZHIGH + row + 3] = v[N - 3 : N]
            for slot, (c, l) in enumerate(PARTS):
                if (c, l) == (comp, layer):
                    to_high[slot] = v
                if (c, 1 - l) == (comp, layer):
                    to_low[slot] = v
    for layer in range(2):
        base = layer * INV
        chunks[0, base : base + 2] = jnp.zeros((2, N), F32)
        chunks[3, base + 130 : base + 132] = jnp.zeros((2, N), F32)
        for j in range(4):
            v = (1.0 / cond[0, layer, :, j * N : (j + 1) * N]).T
            chunks[j, base + 2 : base + 130] = v
            chunks[j, base + 132 : base + INV] = jnp.zeros((4, N), F32)
            if j < 3:
                chunks[j + 1, base : base + 2] = v[N - 2 : N]
            if j > 0:
                chunks[j - 1, base + 130 : base + 132] = v[0:2]
    for q in range(4):
        chunks[q, ZHIGH + 18 : CHUNK] = jnp.zeros((CHUNK - ZHIGH - 18, N), F32)


def z_planes(grp, got, comp, layer):
    row = (comp * 2 + layer) * 3
    low = got[jnp.maximum(grp - 1, 0), ZHIGH + row : ZHIGH + row + 3]
    high = got[jnp.minimum(grp + 1, 3), ZLOW + row : ZLOW + row + 3]
    return jnp.where(grp > 0, low, 0.0), jnp.where(grp < 3, high, 0.0)


def pack(grp_ref, got, to_high, to_low):
    grp = grp_ref[0]
    for out, flip in ((to_high, False), (to_low, True)):
        layer = 0 if flip else 1
        for space in range(4):
            out[space * INV : (space + 1) * INV] = got[space, layer * INV : (layer + 1) * INV]
        for slot, (c, l) in enumerate(PARTS):
            low, high = z_planes(grp, got, c, 1 - l if flip else l)
            row = SIDE + 8 * slot
            out[row : row + 3] = low
            out[row + 3 : row + 6] = high
            out[row + 6 : row + 8] = jnp.zeros((2, N), F32)


def fill_masked(grp, own, got, low_main, high_main, low_side, high_side, m):
    for comp in range(3):
        for layer in range(2):
            low, high = z_planes(grp, got, comp, layer)
            m[layer + 2, comp, 0:3] = low
            m[layer + 2, comp, 3 : 3 + N] = own[comp, layer]
            m[layer + 2, comp, 3 + N : 6 + N] = high
    for main, side, at in ((low_main, low_side, (1, 0)), (high_main, high_side, (4, 5))):
        for slot, (comp, l) in enumerate(PARTS):
            row = SIDE + 8 * slot
            where = at[1 - l]
            m[where, comp, 0:3] = side[row : row + 3]
            m[where, comp, 3 : 3 + N] = main[slot]
            m[where, comp, 3 + N : 6 + N] = side[row + 3 : row + 6]


def restrict_tile(m, place, start, rows):
    def at(layer, comp, shift):
        return m[layer, comp, start + 1 + shift : start + 1 + shift + rows]

    x0, xm, xp = (at(place, 0, s) for s in (0, -1, 1))
    y0, ym, yp = (at(place, 1, s) for s in (0, -1, 1))
    z0 = at(place, 2, 0)
    yl0, ylm, ylp = (at(place - 1, 1, s) for s in (0, -1, 1))
    zl0 = at(place - 1, 2, 0)
    yn0, ynm = (at(place + 1, 1, s) for s in (0, -1))
    zn0 = at(place + 1, 2, 0)
    xsum = x0 + xm
    zsum = z0 + zl0
    curl_x = z0 - from_below(z0) - y0 + ym
    curl_x_next = zn0 - from_below(zn0) - yn0 + ynm
    curl_y = x0 - xm - z0 + zl0
    curl_z = y0 - yl0 - x0 + from_below(x0)
    curl_z_next = yp - ylp - xp + from_below(xp)
    return (
        (x0, y0, z0),
        (
            0.25 * (xsum + from_below(xsum)),
            0.25 * (y0 + ym + (yl0 + ylm)),
            0.25 * (zsum + from_below(zsum)),
        ),
        (curl_x, curl_y, curl_z),
        (
            0.5 * (curl_x + curl_x_next),
            0.5 * (curl_y + from_above(curl_y)),
            0.5 * (curl_z + curl_z_next),
        ),
    )


def correct(
    grp_ref, own, got, low_main, high_main, low_side, high_side, table,
    out, to_high, to_low, m, h, part, w,
):
    grp = grp_ref[0]
    fill_masked(grp, own, got, low_main, high_main, low_side, high_side, m)
    for layer in range(-1, 3):
        for tile in range(HROWS // 8):
            start = 8 * tile
            spaces = restrict_tile(m, layer + 2, start, 8)
            if start >= INV:
                continue
            for space in range(4):
                if layer == -1:
                    inv = low_side[space * INV + start : space * INV + start + 8]
                elif layer == 2:
                    inv = high_side[space * INV + start : space * INV + start + 8]
                else:
                    row = layer * INV + start
                    inv = got[space, row : row + 8]
                for comp in range(3):
                    h[space, comp, layer + 1, start : start + 8] = spaces[space][comp] * inv

    tiles = WROWS // 8

    def finish(step):
        space = step // tiles
        start = pl.multiple_of((step % tiles) * 8, 8)
        for d in range(3):
            for layer in range(2):
                total = part[1, d, layer] + (
                    from_below(part[0, d, layer]) + from_above(part[2, d, layer])
                )
                w[space, d, layer, pl.ds(start, 8)] = total

    def dense(step, carry):
        finish(jnp.maximum(step - 1, 0))
        space = step // tiles
        start = (step % tiles) * 8
        sums = [[[None, None] for d in range(3)] for dy in range(3)]
        for c in range(3):
            for dz in range(3):
                fields = [h[space, c, layer, pl.ds(start + dz, 8)] for layer in range(4)]
                for dx in range(3):
                    for dy in range(3):
                        for d in range(3):
                            index = ((dx * 9 + dy * 3 + dz) * 3 + d) * 3 + c
                            weight = table[pl.ds(space * 243 + index, 8, stride=0)]
                            for layer in range(2):
                                term = weight * fields[layer + dx]
                                old = sums[dy][d][layer]
                                sums[dy][d][layer] = term if old is None else old + term
        for dy in range(3):
            for d in range(3):
                for layer in range(2):
                    part[dy, d, layer] = sums[dy][d][layer]
        return carry

    lax.fori_loop(0, 4 * tiles, dense, 0)
    finish(4 * tiles - 1)

    blank = jnp.zeros((1, N), F32)

    @pl.when(grp == 0)
    def _():
        for space in range(4):
            for d in range(3):
                for layer in range(2):
                    w[space, d, layer, 0:1] = blank

    @pl.when(grp == 3)
    def _():
        for space in range(4):
            for d in range(3):
                for layer in range(2):
                    w[space, d, layer, N + 1 : N + 2] = blank

    to_high[...] = w[3, 0, 1]
    for tile in range(N // 8):
        start = 8 * tile

        def at(space, d, layer, shift):
            return w[space, d, layer, start + 1 + shift : start + 9 + shift]

        def tx(layer, shift):
            total = at(2, 0, layer, shift) + 0.5 * at(3, 0, layer, shift)
            return total + 0.5 * at(3, 0, 0, shift) if layer == 1 else total

        def ty(layer, shift):
            v = at(3, 1, layer, shift)
            return at(2, 1, layer, shift) + 0.5 * (v + from_below(v))

        def tz(layer):
            return at(2, 2, layer, 0) + 0.5 * (at(3, 2, layer, 0) + at(3, 2, layer, -1))

        rows = slice(start, start + 8)
        tys = [ty(layer, 0) for layer in range(2)]
        tzs = [tz(layer) for layer in range(2)]
        ysum = [0.25 * (at(1, 1, layer, 0) + at(1, 1, layer, 1)) for layer in range(2)]
        zsum = []
        for layer in range(2):
            v = at(1, 2, layer, 0)
            zsum.append(0.25 * (v + from_above(v)))
        for layer in range(2):
            xsum = at(1, 0, layer, 0) + at(1, 0, layer, 1)
            out[0, layer, rows] = (
                at(0, 0, layer, 0) + 0.25 * (xsum + from_above(xsum))
                + (tys[layer] - ty(layer, 1)) - (tzs[layer] - from_above(tzs[layer]))
            )
            x_here = tx(layer, 0)
            y_total = at(0, 1, layer, 0) + ysum[layer] + tzs[layer] - (x_here - tx(layer, 1))
            z_total = (
                at(0, 2, layer, 0) + zsum[layer] - tys[layer] + (x_here - from_above(x_here))
            )
            if layer == 0:
                y_total += ysum[1] - tzs[1]
                z_total += zsum[1] + tys[1]
                to_low[0, rows] = ysum[0] - tzs[0]
                to_low[1, rows] = zsum[0] + tys[0]
            out[1, layer, rows] = y_total
            out[2, layer, rows] = z_total


def combine(part, low, high, mask, out):
    g0 = low[1 : 1 + N]
    g1 = low[2 : 2 + N]
    for comp in range(3):
        for layer in range(2):
            v = part[comp, layer]
            if layer == 1 and comp > 0:
                v = v + high[comp - 1]
            if layer == 0 and comp == 1:
                v = v - 0.5 * (g0 - g1)
            if layer == 0 and comp == 2:
                v = v + 0.5 * (g0 - from_above(g0))
            out[comp, layer] = v.T * mask[comp, layer].astype(F32)


def local(residual, face_mask, conductivity, stencil):
    blocks = lax.axis_size("blk")
    up = [(i, i + 1) for i in range(blocks - 1)]
    down = [(i + 1, i) for i in range(blocks - 1)]
    grp = lax.axis_index("grp").astype(jnp.int32).reshape(1)

    step = OMEGA / jnp.diagonal(stencil[:, 13], axis1=1, axis2=2)
    table = -stencil * step[:, None, :, None] * step[:, None, None, :]
    table = table.at[:, 13].add(2.0 * step[:, :, None] * jnp.eye(3, dtype=F32))
    table = jnp.broadcast_to(table.reshape(972, 1), (972, N))

    own, to_high, to_low, chunks = call(
        prepare, "prepare",
        [(3, 2, N, N), (5, N, N), (5, N, N), (4, CHUNK, N)],
        [vmem()] * 3,
    )(residual, face_mask, conductivity)
    low_main = lax.ppermute(to_high, "blk", up)
    high_main = lax.ppermute(to_low, "blk", down)
    got = lax.all_to_all(chunks, "grp", split_axis=0, concat_axis=0, tiled=True)
    to_high, to_low = call(
        pack, "pack", [(MESSAGE, N), (MESSAGE, N)], [smem(), vmem()]
    )(grp, got)
    low_side = lax.ppermute(to_high, "blk", up)
    high_side = lax.ppermute(to_low, "blk", down)
    part, to_high, to_low = call(
        correct, "correct",
        [(3, 2, N, N), (WROWS, N), (2, N, N)],
        [smem()] + [vmem()] * 7,
        [
            pltpu.VMEM((6, 3, MROWS, N), F32),
            pltpu.VMEM((4, 3, 4, HROWS, N), F32),
            pltpu.VMEM((3, 3, 2, 8, N), F32),
            pltpu.VMEM((4, 3, 2, WROWS, N), F32),
        ],
    )(grp, own, got, low_main, high_main, low_side, high_side, table)
    low = lax.ppermute(to_high, "blk", up)
    high = lax.ppermute(to_low, "blk", down)
    (out,) = call(combine, "combine", [(3, 2, N, N)], [vmem()] * 4)(part, low, high, face_mask)
    return out


def solution(mesh):
    return jax.shard_map(
        local,
        mesh=mesh,
        in_specs=(
            P(None, "blk", None, "grp"),
            P(None, "blk", None, "grp"),
            P("grp", "blk", None, None),
            P(),
        ),
        out_specs=P(None, "blk", None, "grp"),
        check_vma=False,
    )
```

```python
import jax
import jax.numpy as jnp
import numpy as np
from jax import lax
from jax.experimental import pallas as pl
from jax.experimental.pallas import tpu as pltpu
from jax.sharding import PartitionSpec as P

OMEGA = 0.8
F32 = jnp.float32
N = 128
INV = 136
ZLOW = 2 * INV
ZHIGH = ZLOW + 18
CHUNK = 312
MROWS = 152
XROWS = 136
HROWS = 144
WROWS = 136
CENTRE = np.zeros((27, 3, 3), np.float32)
CENTRE[13] = 2.0 * np.eye(3)


def vmem():
    return pl.BlockSpec(memory_space=pltpu.VMEM)


def smem():
    return pl.BlockSpec(memory_space=pltpu.SMEM)


def call(kernel, name, out_shapes, in_specs, scratch=()):
    return pl.pallas_call(
        kernel,
        name=name,
        out_shape=[jax.ShapeDtypeStruct(shape, F32) for shape in out_shapes],
        in_specs=in_specs,
        out_specs=[vmem() for _ in out_shapes],
        scratch_shapes=list(scratch),
        compiler_params=pltpu.CompilerParams(vmem_limit_bytes=50 << 20),
    )


def from_below(v):
    lane = lax.broadcasted_iota(jnp.int32, v.shape, 1)
    return jnp.where(lane == 0, 0.0, pltpu.roll(v, 1, 1))


def from_above(v):
    lane = lax.broadcasted_iota(jnp.int32, v.shape, 1)
    return jnp.where(lane == N - 1, 0.0, pltpu.roll(v, N - 1, 1))


def prepare(res_hbm, mask_hbm, cond_hbm, own, chunks, res, mask, cond, sems):
    copies = [
        pltpu.make_async_copy(src, dst, sems.at[i])
        for i, (src, dst) in enumerate(((cond_hbm, cond), (res_hbm, res), (mask_hbm, mask)))
    ]
    for copy in copies:
        copy.start()
    copies[0].wait()
    for layer in range(2):
        base = layer * INV
        chunks[0, base : base + 2] = jnp.zeros((2, N), F32)
        chunks[3, base + 130 : base + 132] = jnp.zeros((2, N), F32)
        for j in range(4):
            v = (1.0 / cond[0, layer, :, j * N : (j + 1) * N]).T
            chunks[j, base + 2 : base + 130] = v
            chunks[j, base + 132 : base + INV] = jnp.zeros((4, N), F32)
            if j < 3:
                chunks[j + 1, base : base + 2] = v[N - 2 : N]
            if j > 0:
                chunks[j - 1, base + 130 : base + 132] = v[0:2]
    for q in range(4):
        chunks[q, ZHIGH + 18 : CHUNK] = jnp.zeros((CHUNK - ZHIGH - 18, N), F32)
    copies[1].wait()
    copies[2].wait()
    for comp in range(3):
        for layer in range(2):
            v = (res[comp, layer] * mask[comp, layer].astype(F32)).T
            own[comp, layer] = v
            row = (comp * 2 + layer) * 3
            for q in range(4):
                chunks[q, ZLOW + row : ZLOW + row + 3] = v[0:3]
                chunks[q, ZHIGH + row : ZHIGH + row + 3] = v[N - 3 : N]


def z_planes(grp, got, comp, layer):
    row = (comp * 2 + layer) * 3
    low = got[jnp.maximum(grp - 1, 0), pl.ds(ZHIGH + row, 3)]
    high = got[jnp.minimum(grp + 1, 3), pl.ds(ZLOW + row, 3)]
    return jnp.where(grp > 0, low, 0.0), jnp.where(grp < 3, high, 0.0)


def pack(place, own, got, table, first, second):
    grp = place[0]
    odd = place[1] % 2
    for out, layer in ((first, odd), (second, 1 - odd)):
        for slot in range(2):
            low, high = z_planes(grp, got, slot + 1, layer)
            row = slot * XROWS
            out[row : row + 3] = low
            out[row + 3 : row + 3 + N] = own[slot + 1, layer]
            out[row + 3 + N : row + 6 + N] = high
            out[row + 6 + N : row + XROWS] = jnp.zeros((2, N), F32)


def fill_masked(grp, odd, own, got, first, second, m):
    for comp in range(3):
        for layer in range(2):
            low, high = z_planes(grp, got, comp, layer)
            m[layer + 1, comp, 0:3] = low
            m[layer + 1, comp, 3 : 3 + N] = own[comp, layer]
            m[layer + 1, comp, 3 + N : 6 + N] = high
    for got_x, where in ((first, 3 * odd), (second, 3 * (1 - odd))):
        for slot in range(2):
            m[where, slot + 1, 0:XROWS] = got_x[slot * XROWS : (slot + 1) * XROWS]


def restrict_tile(m, place, start, rows):
    def at(layer, comp, shift):
        return m[layer, comp, start + 1 + shift : start + 1 + shift + rows]

    x0, xm, xp = (at(place, 0, s) for s in (0, -1, 1))
    y0, ym, yp = (at(place, 1, s) for s in (0, -1, 1))
    z0 = at(place, 2, 0)
    yl0, ylm, ylp = (at(place - 1, 1, s) for s in (0, -1, 1))
    zl0 = at(place - 1, 2, 0)
    yn0, ynm = (at(place + 1, 1, s) for s in (0, -1))
    zn0 = at(place + 1, 2, 0)
    xsum = x0 + xm
    zsum = z0 + zl0
    curl_x = z0 - from_below(z0) - y0 + ym
    curl_x_next = zn0 - from_below(zn0) - yn0 + ynm
    curl_y = x0 - xm - z0 + zl0
    curl_z = y0 - yl0 - x0 + from_below(x0)
    curl_z_next = yp - ylp - xp + from_below(xp)
    return (
        (x0, y0, z0),
        (
            0.25 * (xsum + from_below(xsum)),
            0.25 * (y0 + ym + (yl0 + ylm)),
            0.25 * (zsum + from_below(zsum)),
        ),
        (curl_x, curl_y, curl_z),
        (
            0.5 * (curl_x + curl_x_next),
            0.5 * (curl_y + from_above(curl_y)),
            0.5 * (curl_z + curl_z_next),
        ),
    )


def correct(place, own, got, first_x, second_x, table, out, first, second, m, h, part, w, sent):
    grp = place[0]
    blk = place[1]
    odd = blk % 2
    fill_masked(grp, odd, own, got, first_x, second_x, m)
    for layer in range(2):
        for tile in range(INV // 8):
            start = 8 * tile
            spaces = restrict_tile(m, layer + 1, start, 8)
            for space in range(4):
                row = layer * INV + start
                inv = got[space, row : row + 8]
                for comp in range(3):
                    h[space, comp, layer, start : start + 8] = spaces[space][comp] * inv

    tiles = WROWS // 8

    def finish(step):
        space = step // tiles
        start = pl.multiple_of((step % tiles) * 8, 8)
        for d in range(3):
            for layer in range(4):
                total = part[1, d, layer] + (
                    from_below(part[0, d, layer]) + from_above(part[2, d, layer])
                )
                w[space, d, layer, pl.ds(start, 8)] = total

    def dense(step, carry):
        finish(jnp.maximum(step - 1, 0))
        space = step // tiles
        start = (step % tiles) * 8
        for dy in range(3):
            sums = [[None] * 4 for d in range(3)]
            for c in range(3):
                for dz in range(3):
                    fields = [h[space, c, layer, pl.ds(start + dz, 8)] for layer in range(2)]
                    for dx in range(3):
                        for d in range(3):
                            index = ((dx * 9 + dy * 3 + dz) * 3 + d) * 3 + c
                            weight = table[pl.ds(space * 243 + index, 8, stride=0)]
                            for layer in range(2):
                                to = layer + 2 - dx
                                term = weight * fields[layer]
                                old = sums[d][to]
                                sums[d][to] = term if old is None else old + term
            for d in range(3):
                for to in range(4):
                    part[dy, d, to] = sums[d][to]
        return carry

    lax.fori_loop(0, 4 * tiles, dense, 0)
    finish(4 * tiles - 1)

    def clear(layers, rows):
        for space in range(4):
            for d in range(3):
                for layer in layers:
                    w[space, d, layer, rows] = jnp.zeros((rows.stop - rows.start, N), F32)

    @pl.when(grp == 0)
    def _():
        clear(range(4), slice(0, 1))

    @pl.when(grp == 3)
    def _():
        clear(range(4), slice(N + 1, N + 2))

    @pl.when(blk == 0)
    def _():
        clear((0,), slice(0, WROWS))

    @pl.when(blk == place[2])
    def _():
        clear((3,), slice(0, WROWS))

    for tile in range(N // 8):
        start = 8 * tile
        rows = slice(start, start + 8)

        def at(space, d, layer, shift):
            return w[space, d, layer, start + 1 + shift : start + 9 + shift]

        def along_x(shift):
            half = [0.5 * at(3, 0, layer, shift) for layer in range(4)]
            inner = [at(2, 0, layer, shift) + half[layer] for layer in range(4)]
            return [inner[0]] + [inner[i] + half[i - 1] for i in (1, 2, 3)] + [half[3]]

        def along_y(layer, shift):
            v = at(3, 1, layer, shift)
            return at(2, 1, layer, shift) + 0.5 * (v + from_below(v))

        def along_z(layer):
            return at(2, 2, layer, 0) + 0.5 * (at(3, 2, layer, 0) + at(3, 2, layer, -1))

        tx = along_x(0)
        tx_next = along_x(1)
        ty = [along_y(layer, 0) for layer in range(4)]
        tz = [along_z(layer) for layer in range(4)]
        y_sum = [0.25 * (at(1, 1, layer, 0) + at(1, 1, layer, 1)) for layer in range(4)]
        z_own = [at(1, 2, layer, 0) for layer in range(4)]
        z_sum = [0.25 * (v + from_above(v)) for v in z_own]
        xs, ys, zs = [], [], []
        for layer in range(4):
            x_sum = at(1, 0, layer, 0) + at(1, 0, layer, 1)
            xs.append(
                at(0, 0, layer, 0) + 0.25 * (x_sum + from_above(x_sum))
                + (ty[layer] - along_y(layer, 1)) - (tz[layer] - from_above(tz[layer]))
            )
        for layer in range(-1, 5):
            y = z = None
            if layer >= 0:
                y = tx_next[layer] - tx[layer]
                z = tx[layer] - from_above(tx[layer])
            if 0 <= layer < 4:
                y = y + (at(0, 1, layer, 0) + y_sum[layer] + tz[layer])
                z = z + (at(0, 2, layer, 0) + z_sum[layer] - ty[layer])
            if layer < 3:
                y_more = y_sum[layer + 1] - tz[layer + 1]
                z_more = z_sum[layer + 1] + ty[layer + 1]
                y = y_more if y is None else y + y_more
                z = z_more if z is None else z + z_more
            ys.append(y)
            zs.append(z)
        for layer in range(2):
            out[0, layer, rows] = xs[layer + 1]
            out[1, layer, rows] = ys[layer + 2]
            out[2, layer, rows] = zs[layer + 2]
        up = (xs[3], ys[4], zs[4], ys[5], zs[5])
        down = (xs[0], ys[1], zs[1], ys[0], zs[0])
        for slot in range(5):
            sent[1 - odd, slot, rows] = up[slot]
            sent[odd, slot, rows] = down[slot]
    first[...] = sent[0]
    second[...] = sent[1]


def combine(place, part, first, second, mask, out, total):
    odd = place[1] % 2
    other = 1 - odd
    for comp in range(3):
        total[comp, odd] = part[comp, odd] + first[comp]
        total[comp, other] = part[comp, other] + second[comp]
    for comp in (1, 2):
        total[comp, odd] += second[comp + 2]
        total[comp, other] += first[comp + 2]
    for comp in range(3):
        for layer in range(2):
            out[comp, layer] = total[comp, layer].T * mask[comp, layer].astype(F32)


def local(residual, face_mask, conductivity, stencil):
    blocks = lax.axis_size("blk")

    def exchange(first, second):
        arrived = []
        for part, begin in ((first, 1), (second, 0)):
            pairs = [(i, i + 1) for i in range(begin, blocks - 1, 2)]
            pairs += [(j, i) for i, j in pairs]
            arrived.append(lax.ppermute(part, "blk", pairs))
        return arrived

    place = jnp.stack(
        [lax.axis_index("grp"), lax.axis_index("blk"), jnp.int32(blocks - 1)]
    ).astype(jnp.int32)

    step = OMEGA / (stencil[:, 13] * np.eye(3, dtype=np.float32)).sum(2)
    table = step[:, None, :, None] * (CENTRE - stencil * step[:, None, None, :])
    table = jnp.broadcast_to(table.reshape(972, 1), (972, N))

    own, chunks = call(
        prepare, "prepare",
        [(3, 2, N, N), (4, CHUNK, N)],
        [pl.BlockSpec(memory_space=pltpu.HBM)] * 3,
        [
            pltpu.VMEM((3, 2, N, N), F32),
            pltpu.VMEM((3, 2, N, N), jnp.int32),
            pltpu.VMEM((1, 2, N, 4 * N), F32),
            pltpu.SemaphoreType.DMA((3,)),
        ],
    )(*(
        pltpu.with_memory_space_constraint(v, pltpu.HBM)
        for v in (residual, face_mask, conductivity)
    ))
    got = lax.all_to_all(chunks, "grp", split_axis=0, concat_axis=0, tiled=True)
    first, second = call(
        pack, "pack", [(2 * XROWS, N)] * 2, [smem()] + [vmem()] * 3
    )(place, own, got, table)
    first, second = exchange(first, second)
    part, first, second = call(
        correct, "correct",
        [(3, 2, N, N), (5, N, N), (5, N, N)],
        [smem()] + [vmem()] * 5,
        [
            pltpu.VMEM((4, 3, MROWS, N), F32),
            pltpu.VMEM((4, 3, 2, HROWS, N), F32),
            pltpu.VMEM((3, 3, 4, 8, N), F32),
            pltpu.VMEM((4, 3, 4, WROWS, N), F32),
            pltpu.VMEM((2, 5, N, N), F32),
        ],
    )(place, own, got, first, second, table)
    first, second = exchange(first, second)
    (out,) = call(
        combine, "combine", [(3, 2, N, N)], [smem()] + [vmem()] * 4,
        [pltpu.VMEM((3, 2, N, N), F32)],
    )(place, part, first, second, face_mask)
    return out


def solution(mesh):
    return jax.shard_map(
        local,
        mesh=mesh,
        in_specs=(
            P(None, "blk", None, "grp"),
            P(None, "blk", None, "grp"),
            P("grp", "blk", None, None),
            P(),
        ),
        out_specs=P(None, "blk", None, "grp"),
        check_vma=False,
    )
```

```python
import jax
import jax.numpy as jnp
import numpy as np
from jax import lax
from jax.experimental import pallas as pl
from jax.experimental.pallas import tpu as pltpu
from jax.sharding import PartitionSpec as P

OMEGA = 0.8
F32 = jnp.float32
N = 128
INV = 136
PLANES = 24
MROWS = 144
XROWS = 136
HROWS = 144
WROWS = 136
CENTRE = np.zeros((27, 3, 3), np.float32)
CENTRE[13] = 2.0 * np.eye(3)


def vmem():
    return pl.BlockSpec(memory_space=pltpu.VMEM)


def smem():
    return pl.BlockSpec(memory_space=pltpu.SMEM)


def call(kernel, name, out_shapes, in_specs, scratch=()):
    return pl.pallas_call(
        kernel,
        name=name,
        out_shape=[jax.ShapeDtypeStruct(shape, F32) for shape in out_shapes],
        in_specs=in_specs,
        out_specs=[vmem() for _ in out_shapes],
        scratch_shapes=list(scratch),
        compiler_params=pltpu.CompilerParams(vmem_limit_bytes=50 << 20),
    )


def from_below(v):
    lane = lax.broadcasted_iota(jnp.int32, v.shape, 1)
    return jnp.where(lane == 0, 0.0, pltpu.roll(v, 1, 1))


def from_above(v):
    lane = lax.broadcasted_iota(jnp.int32, v.shape, 1)
    return jnp.where(lane == N - 1, 0.0, pltpu.roll(v, N - 1, 1))


def mask_residual(place, res_hbm, mask_hbm, own, first, second, res, mask, planes, sems):
    odd = place[0] % 2
    copies = [
        pltpu.make_async_copy(src, dst, sems.at[i])
        for i, (src, dst) in enumerate(((res_hbm, res), (mask_hbm, mask)))
    ]
    for copy in copies:
        copy.start()
    for copy in copies:
        copy.wait()
    planes[:, 18:PLANES] = jnp.zeros((2, PLANES - 18, N), F32)
    for comp in range(3):
        for layer in range(2):
            v = (res[comp, layer] * mask[comp, layer].astype(F32)).T
            own[comp, layer] = v
            row = (comp * 2 + layer) * 3
            planes[0, row : row + 3] = v[0:3]
            planes[1, row : row + 3] = v[N - 3 : N]
    first[...] = planes[odd]
    second[...] = planes[1 - odd]


def invert(cond_hbm, chunks, cond, sem):
    copy = pltpu.make_async_copy(cond_hbm, cond, sem)
    copy.start()
    copy.wait()
    for layer in range(2):
        base = layer * INV
        chunks[0, base : base + 2] = jnp.zeros((2, N), F32)
        chunks[3, base + 130 : base + 132] = jnp.zeros((2, N), F32)
        for j in range(4):
            v = (1.0 / cond[0, layer, :, j * N : (j + 1) * N]).T
            chunks[j, base + 2 : base + 130] = v
            chunks[j, base + 132 : base + INV] = jnp.zeros((4, N), F32)
            if j < 3:
                chunks[j + 1, base : base + 2] = v[N - 2 : N]
            if j > 0:
                chunks[j - 1, base + 130 : base + 132] = v[0:2]


def pack(place, own, z_first, z_second, field, first, second, planes):
    z_odd = place[0] % 2
    odd = place[1] % 2
    planes[0] = z_first[...]
    planes[1] = z_second[...]
    for layer in range(2):
        for comp in range(3):
            row = (comp * 2 + layer) * 3
            field[layer, comp, 0:3] = planes[z_odd, row : row + 3]
            field[layer, comp, 3 : 3 + N] = own[comp, layer]
            field[layer, comp, 3 + N : 6 + N] = planes[1 - z_odd, row : row + 3]
            field[layer, comp, 6 + N : MROWS] = jnp.zeros((MROWS - N - 6, N), F32)
    for out, layer in ((first, odd), (second, 1 - odd)):
        for slot in range(2):
            out[slot] = field[layer, slot + 1, 0:XROWS]


def restrict_tile(field, side, place, start, rows):
    def at(layer, comp, shift):
        rows_at = slice(start + 1 + shift, start + 1 + shift + rows)
        if layer in (1, 2):
            return field[layer - 1, comp, rows_at]
        return side[layer // 3, comp - 1, rows_at]

    x0, xm, xp = (at(place, 0, s) for s in (0, -1, 1))
    y0, ym, yp = (at(place, 1, s) for s in (0, -1, 1))
    z0 = at(place, 2, 0)
    yl0, ylm, ylp = (at(place - 1, 1, s) for s in (0, -1, 1))
    zl0 = at(place - 1, 2, 0)
    yn0, ynm = (at(place + 1, 1, s) for s in (0, -1))
    zn0 = at(place + 1, 2, 0)
    xsum = x0 + xm
    zsum = z0 + zl0
    curl_x = z0 - from_below(z0) - y0 + ym
    curl_x_next = zn0 - from_below(zn0) - yn0 + ynm
    curl_y = x0 - xm - z0 + zl0
    curl_z = y0 - yl0 - x0 + from_below(x0)
    curl_z_next = yp - ylp - xp + from_below(xp)
    return (
        (x0, y0, z0),
        (
            0.25 * (xsum + from_below(xsum)),
            0.25 * (y0 + ym + (yl0 + ylm)),
            0.25 * (zsum + from_below(zsum)),
        ),
        (curl_x, curl_y, curl_z),
        (
            0.5 * (curl_x + curl_x_next),
            0.5 * (curl_y + from_above(curl_y)),
            0.5 * (curl_z + curl_z_next),
        ),
    )


def correct(
    place, field, got, first_x, second_x, table, out, first, second, side, h, part, w, sent
):
    grp = place[0]
    blk = place[1]
    odd = blk % 2
    for arrived, where in ((first_x, odd), (second_x, 1 - odd)):
        side[where, :, 0:XROWS] = arrived[...]
        side[where, :, XROWS:MROWS] = jnp.zeros((2, MROWS - XROWS, N), F32)
    for layer in range(2):
        for tile in range(INV // 8):
            start = 8 * tile
            spaces = restrict_tile(field, side, layer + 1, start, 8)
            for space in range(4):
                row = layer * INV + start
                inv = got[space, row : row + 8]
                for comp in range(3):
                    h[space, comp, layer, start : start + 8] = spaces[space][comp] * inv

    tiles = WROWS // 8

    def finish(step):
        space = step // tiles
        start = pl.multiple_of((step % tiles) * 8, 8)
        for d in range(3):
            for layer in range(4):
                total = part[1, d, layer] + (
                    from_below(part[0, d, layer]) + from_above(part[2, d, layer])
                )
                w[space, d, layer, pl.ds(start, 8)] = total

    def dense(step, carry):
        finish(jnp.maximum(step - 1, 0))
        space = step // tiles
        start = (step % tiles) * 8
        for dy in range(3):
            sums = [[None] * 4 for d in range(3)]
            for c in range(3):
                for dz in range(3):
                    fields = [h[space, c, layer, pl.ds(start + dz, 8)] for layer in range(2)]
                    for dx in range(3):
                        for d in range(3):
                            index = ((dx * 9 + dy * 3 + dz) * 3 + d) * 3 + c
                            weight = table[pl.ds(space * 243 + index, 8, stride=0)]
                            for layer in range(2):
                                to = layer + 2 - dx
                                term = weight * fields[layer]
                                old = sums[d][to]
                                sums[d][to] = term if old is None else old + term
            for d in range(3):
                for to in range(4):
                    part[dy, d, to] = sums[d][to]
        return carry

    lax.fori_loop(0, 4 * tiles, dense, 0)
    finish(4 * tiles - 1)

    def clear(layers, rows):
        for space in range(4):
            for d in range(3):
                for layer in layers:
                    w[space, d, layer, rows] = jnp.zeros((rows.stop - rows.start, N), F32)

    @pl.when(grp == 0)
    def _():
        clear(range(4), slice(0, 1))

    @pl.when(grp == 3)
    def _():
        clear(range(4), slice(N + 1, N + 2))

    @pl.when(blk == 0)
    def _():
        clear((0,), slice(0, WROWS))

    @pl.when(blk == place[2])
    def _():
        clear((3,), slice(0, WROWS))

    for tile in range(N // 8):
        start = 8 * tile
        rows = slice(start, start + 8)

        def at(space, d, layer, shift):
            return w[space, d, layer, start + 1 + shift : start + 9 + shift]

        def along_x(shift):
            half = [0.5 * at(3, 0, layer, shift) for layer in range(4)]
            inner = [at(2, 0, layer, shift) + half[layer] for layer in range(4)]
            return [inner[0]] + [inner[i] + half[i - 1] for i in (1, 2, 3)] + [half[3]]

        def along_y(layer, shift):
            v = at(3, 1, layer, shift)
            return at(2, 1, layer, shift) + 0.5 * (v + from_below(v))

        def along_z(layer):
            return at(2, 2, layer, 0) + 0.5 * (at(3, 2, layer, 0) + at(3, 2, layer, -1))

        tx = along_x(0)
        tx_next = along_x(1)
        ty = [along_y(layer, 0) for layer in range(4)]
        tz = [along_z(layer) for layer in range(4)]
        y_sum = [0.25 * (at(1, 1, layer, 0) + at(1, 1, layer, 1)) for layer in range(4)]
        z_own = [at(1, 2, layer, 0) for layer in range(4)]
        z_sum = [0.25 * (v + from_above(v)) for v in z_own]
        xs, ys, zs = [], [], []
        for layer in range(4):
            x_sum = at(1, 0, layer, 0) + at(1, 0, layer, 1)
            xs.append(
                at(0, 0, layer, 0) + 0.25 * (x_sum + from_above(x_sum))
                + (ty[layer] - along_y(layer, 1)) - (tz[layer] - from_above(tz[layer]))
            )
        for layer in range(-1, 5):
            y = z = None
            if layer >= 0:
                y = tx_next[layer] - tx[layer]
                z = tx[layer] - from_above(tx[layer])
            if 0 <= layer < 4:
                y = y + (at(0, 1, layer, 0) + y_sum[layer] + tz[layer])
                z = z + (at(0, 2, layer, 0) + z_sum[layer] - ty[layer])
            if layer < 3:
                y_more = y_sum[layer + 1] - tz[layer + 1]
                z_more = z_sum[layer + 1] + ty[layer + 1]
                y = y_more if y is None else y + y_more
                z = z_more if z is None else z + z_more
            ys.append(y)
            zs.append(z)
        for layer in range(2):
            out[0, layer, rows] = xs[layer + 1]
            out[1, layer, rows] = ys[layer + 2]
            out[2, layer, rows] = zs[layer + 2]
        up = (xs[3], ys[4], zs[4], ys[5], zs[5])
        down = (xs[0], ys[1], zs[1], ys[0], zs[0])
        for slot in range(5):
            sent[1 - odd, slot, rows] = up[slot]
            sent[odd, slot, rows] = down[slot]
    first[...] = sent[0]
    second[...] = sent[1]


def combine(place, part, first, second, mask, out, total):
    odd = place[1] % 2
    other = 1 - odd
    for comp in range(3):
        total[comp, odd] = part[comp, odd] + first[comp]
        total[comp, other] = part[comp, other] + second[comp]
    for comp in (1, 2):
        total[comp, odd] += second[comp + 2]
        total[comp, other] += first[comp + 2]
    for comp in range(3):
        for layer in range(2):
            out[comp, layer] = total[comp, layer].T * mask[comp, layer].astype(F32)


def local(residual, face_mask, conductivity, stencil):
    blocks = lax.axis_size("blk")

    def exchange(axis, first, second):
        size = lax.axis_size(axis)
        arrived = []
        for part, begin in ((first, 1), (second, 0)):
            pairs = [(i, i + 1) for i in range(begin, size - 1, 2)]
            pairs += [(j, i) for i, j in pairs]
            arrived.append(lax.ppermute(part, axis, pairs))
        return arrived

    place = jnp.stack(
        [lax.axis_index("grp"), lax.axis_index("blk"), jnp.int32(blocks - 1)]
    ).astype(jnp.int32)

    step = OMEGA / (stencil[:, 13] * np.eye(3, dtype=np.float32)).sum(2)
    table = step[:, None, :, None] * (CENTRE - stencil * step[:, None, None, :])
    table = jnp.broadcast_to(table.reshape(972, 1), (972, N))

    in_hbm = pl.BlockSpec(memory_space=pltpu.HBM)
    residual, mask, conductivity = (
        pltpu.with_memory_space_constraint(v, pltpu.HBM)
        for v in (residual, face_mask, conductivity)
    )
    own, first, second = call(
        mask_residual, "mask_residual",
        [(3, 2, N, N), (PLANES, N), (PLANES, N)],
        [smem(), in_hbm, in_hbm],
        [
            pltpu.VMEM((3, 2, N, N), F32),
            pltpu.VMEM((3, 2, N, N), jnp.int32),
            pltpu.VMEM((2, PLANES, N), F32),
            pltpu.SemaphoreType.DMA((2,)),
        ],
    )(place, residual, mask)
    z_first, z_second = exchange("grp", first, second)
    (chunks,) = call(
        invert, "invert", [(4, 2 * INV, N)], [in_hbm],
        [pltpu.VMEM((1, 2, N, 4 * N), F32), pltpu.SemaphoreType.DMA(())],
    )(conductivity)
    got = lax.all_to_all(chunks, "grp", split_axis=0, concat_axis=0, tiled=True)
    field, first, second = call(
        pack, "pack",
        [(2, 3, MROWS, N), (2, XROWS, N), (2, XROWS, N)],
        [smem()] + [vmem()] * 3,
        [pltpu.VMEM((2, PLANES, N), F32)],
    )(place, own, z_first, z_second)
    first, second = exchange("blk", first, second)
    part, first, second = call(
        correct, "correct",
        [(3, 2, N, N), (5, N, N), (5, N, N)],
        [smem()] + [vmem()] * 5,
        [
            pltpu.VMEM((2, 2, MROWS, N), F32),
            pltpu.VMEM((4, 3, 2, HROWS, N), F32),
            pltpu.VMEM((3, 3, 4, 8, N), F32),
            pltpu.VMEM((4, 3, 4, WROWS, N), F32),
            pltpu.VMEM((2, 5, N, N), F32),
        ],
    )(place, field, got, first, second, table)
    first, second = exchange("blk", first, second)
    (out,) = call(
        combine, "combine", [(3, 2, N, N)], [smem()] + [vmem()] * 4,
        [pltpu.VMEM((3, 2, N, N), F32)],
    )(place, part, first, second, face_mask)
    return out


def solution(mesh):
    return jax.shard_map(
        local,
        mesh=mesh,
        in_specs=(
            P(None, "blk", None, "grp"),
            P(None, "blk", None, "grp"),
            P("grp", "blk", None, None),
            P(),
        ),
        out_specs=P(None, "blk", None, "grp"),
        check_vma=False,
    )
```

```python
import jax
import jax.numpy as jnp
import numpy as np
from jax import lax
from jax.experimental import pallas as pl
from jax.experimental.pallas import tpu as pltpu
from jax.sharding import PartitionSpec as P

OMEGA = 0.8
F32 = jnp.float32
BF16 = jnp.bfloat16
N = 128
INV = 136
PLANES = 24
MROWS = 144
XROWS = 136
HROWS = 144
WROWS = 136
BLOCK = 6
PAIRS = 11
TERM = 48
DEPTH = 3 * TERM
CENTRE = np.zeros((27, 3, 3), np.float32)
CENTRE[13] = 2.0 * np.eye(3)


def vmem():
    return pl.BlockSpec(memory_space=pltpu.VMEM)


def smem():
    return pl.BlockSpec(memory_space=pltpu.SMEM)


def call(kernel, name, out_shapes, in_specs, scratch=(), dtype=F32):
    return pl.pallas_call(
        kernel,
        name=name,
        out_shape=[jax.ShapeDtypeStruct(shape, dtype) for shape in out_shapes],
        in_specs=in_specs,
        out_specs=[vmem() for _ in out_shapes],
        scratch_shapes=list(scratch),
        compiler_params=pltpu.CompilerParams(vmem_limit_bytes=50 << 20),
    )


def from_below(v):
    lane = lax.broadcasted_iota(jnp.int32, v.shape, 1)
    return jnp.where(lane == 0, 0.0, pltpu.roll(v, 1, 1))


def from_above(v):
    lane = lax.broadcasted_iota(jnp.int32, v.shape, 1)
    return jnp.where(lane == N - 1, 0.0, pltpu.roll(v, N - 1, 1))


def mask_residual(place, res_hbm, mask_hbm, own, first, second, res, mask, planes, sems):
    odd = place[0] % 2
    copies = [
        pltpu.make_async_copy(src, dst, sems.at[i])
        for i, (src, dst) in enumerate(((res_hbm, res), (mask_hbm, mask)))
    ]
    for copy in copies:
        copy.start()
    for copy in copies:
        copy.wait()
    planes[:, 18:PLANES] = jnp.zeros((2, PLANES - 18, N), F32)
    for comp in range(3):
        for layer in range(2):
            v = (res[comp, layer] * mask[comp, layer].astype(F32)).T
            own[comp, layer] = v
            row = (comp * 2 + layer) * 3
            planes[0, row : row + 3] = v[0:3]
            planes[1, row : row + 3] = v[N - 3 : N]
    first[...] = planes[odd]
    second[...] = planes[1 - odd]


def invert(cond_hbm, chunks, cond, sem):
    copy = pltpu.make_async_copy(cond_hbm, cond, sem)
    copy.start()
    copy.wait()
    for layer in range(2):
        base = layer * INV
        chunks[0, base : base + 2] = jnp.zeros((2, N), F32)
        chunks[3, base + 130 : base + 132] = jnp.zeros((2, N), F32)
        for j in range(4):
            v = (1.0 / cond[0, layer, :, j * N : (j + 1) * N]).T
            chunks[j, base + 2 : base + 130] = v
            chunks[j, base + 132 : base + INV] = jnp.zeros((4, N), F32)
            if j < 3:
                chunks[j + 1, base : base + 2] = v[N - 2 : N]
            if j > 0:
                chunks[j - 1, base + 130 : base + 132] = v[0:2]


def pack(place, own, z_first, z_second, field, first, second, planes):
    z_odd = place[0] % 2
    odd = place[1] % 2
    planes[0] = z_first[...]
    planes[1] = z_second[...]
    for layer in range(2):
        for comp in range(3):
            row = (comp * 2 + layer) * 3
            field[layer, comp, 0:3] = planes[z_odd, row : row + 3]
            field[layer, comp, 3 : 3 + N] = own[comp, layer]
            field[layer, comp, 3 + N : 6 + N] = planes[1 - z_odd, row : row + 3]
            field[layer, comp, 6 + N : MROWS] = jnp.zeros((MROWS - N - 6, N), F32)
    for out, layer in ((first, odd), (second, 1 - odd)):
        for slot in range(2):
            out[slot] = field[layer, slot + 1, 0:XROWS]


def restrict_tile(field, side, place, start, rows):
    def at(layer, comp, shift):
        rows_at = slice(start + 1 + shift, start + 1 + shift + rows)
        if layer in (1, 2):
            return field[layer - 1, comp, rows_at]
        return side[layer // 3, comp - 1, rows_at]

    x0, xm, xp = (at(place, 0, s) for s in (0, -1, 1))
    y0, ym, yp = (at(place, 1, s) for s in (0, -1, 1))
    z0 = at(place, 2, 0)
    yl0, ylm, ylp = (at(place - 1, 1, s) for s in (0, -1, 1))
    zl0 = at(place - 1, 2, 0)
    yn0, ynm = (at(place + 1, 1, s) for s in (0, -1))
    zn0 = at(place + 1, 2, 0)
    xsum = x0 + xm
    zsum = z0 + zl0
    curl_x = z0 - from_below(z0) - y0 + ym
    curl_x_next = zn0 - from_below(zn0) - yn0 + ynm
    curl_y = x0 - xm - z0 + zl0
    curl_z = y0 - yl0 - x0 + from_below(x0)
    curl_z_next = yp - ylp - xp + from_below(xp)
    return (
        (x0, y0, z0),
        (
            0.25 * (xsum + from_below(xsum)),
            0.25 * (y0 + ym + (yl0 + ylm)),
            0.25 * (zsum + from_below(zsum)),
        ),
        (curl_x, curl_y, curl_z),
        (
            0.5 * (curl_x + curl_x_next),
            0.5 * (curl_y + from_above(curl_y)),
            0.5 * (curl_z + curl_z_next),
        ),
    )


def band(table, out):
    row = lax.broadcasted_iota(jnp.int32, (8, N), 0)
    lane = lax.broadcasted_iota(jnp.int32, (8, N), 1)

    def codes(at):
        term = (at >= TERM).astype(jnp.int32) + (at >= 2 * TERM).astype(jnp.int32)
        k = at - TERM * term
        dz = (k & 7) - row
        fits = (at < DEPTH) & (row < BLOCK) & (dz >= 0) & (dz < 3)
        return jnp.where(fits, (k >> 3) * 8 + dz, -1)

    code = (codes(lane), codes(lane + N))

    def fill(step, carry):
        space = step // 9
        entry = step % 9
        dy = entry // 3
        d = entry % 3
        rows = []
        for to in range(4):
            halves = [jnp.zeros((8, N), F32), jnp.zeros((8, N), F32)]
            for layer in range(2):
                dx = layer + 2 - to
                if dx < 0 or dx > 2:
                    continue
                for c in range(3):
                    for dz in range(3):
                        index = ((space * 27 + dx * 9 + dy * 3 + dz) * 3 + d) * 3 + c
                        value = table[pl.ds(index, 8, stride=0)]
                        for half in range(2 if c == 2 else 1):
                            hit = code[half] == (c * 2 + layer) * 8 + dz
                            halves[half] = jnp.where(hit, value, halves[half])
            parts = []
            for half, v in enumerate(halves):
                high = v.astype(BF16).astype(F32)
                parts.append(jnp.where(lane + half * N < 2 * TERM, high, v - high))
            rows.append(jnp.concatenate(parts, 1))
        start = pl.multiple_of(entry * 32, 32)
        out[space, pl.ds(start, 32)] = jnp.concatenate(rows, 0).astype(BF16)
        return carry

    lax.fori_loop(0, 36, fill, 0)


def correct(
    place, field, got, first_x, second_x, weights, out, first, second, side, h, w, sent
):
    grp = place[0]
    blk = place[1]
    odd = blk % 2
    for arrived, where in ((first_x, odd), (second_x, 1 - odd)):
        side[where, :, 0:XROWS] = arrived[...]
        side[where, :, XROWS:MROWS] = jnp.zeros((2, MROWS - XROWS, N), F32)
    for layer in range(2):
        for tile in range(INV // 8):
            start = 8 * tile
            spaces = restrict_tile(field, side, layer + 1, start, 8)
            for space in range(4):
                row = layer * INV + start
                inv = got[space, row : row + 8]
                for comp in range(3):
                    h[space, comp, layer, start : start + 8] = spaces[space][comp] * inv

    def dense(space, carry):
        for pair in range(PAIRS):
            starts = (2 * BLOCK * pair, 2 * BLOCK * pair + BLOCK)
            fields = jnp.concatenate([
                jnp.concatenate(
                    [h[space, c, layer, at : at + 8] for c in range(3) for layer in range(2)], 0
                )
                for at in starts
            ], 1)
            high = fields.astype(BF16)
            low = (fields - high.astype(F32)).astype(BF16)
            sums = jnp.dot(
                weights[space, :, 0:DEPTH],
                jnp.concatenate([high, low, high], 0),
                preferred_element_type=F32,
            )
            for half, at in enumerate(starts):
                lanes = slice(half * N, half * N + N)
                for d in range(3):
                    for to in range(4):
                        below, here, above = (
                            sums[row * 8 : row * 8 + 8, lanes]
                            for row in ((dy * 3 + d) * 4 + to for dy in range(3))
                        )
                        w[space, d, to, at : at + 8] = here + (
                            from_below(below) + from_above(above)
                        )
        return carry

    lax.fori_loop(0, 4, dense, 0)

    def clear(layers, rows):
        for space in range(4):
            for d in range(3):
                for layer in layers:
                    w[space, d, layer, rows] = jnp.zeros((rows.stop - rows.start, N), F32)

    @pl.when(grp == 0)
    def _():
        clear(range(4), slice(0, 1))

    @pl.when(grp == 3)
    def _():
        clear(range(4), slice(N + 1, N + 2))

    @pl.when(blk == 0)
    def _():
        clear((0,), slice(0, WROWS))

    @pl.when(blk == place[2])
    def _():
        clear((3,), slice(0, WROWS))

    for tile in range(N // 8):
        start = 8 * tile
        rows = slice(start, start + 8)

        def at(space, d, layer, shift):
            return w[space, d, layer, start + 1 + shift : start + 9 + shift]

        def along_x(shift):
            half = [0.5 * at(3, 0, layer, shift) for layer in range(4)]
            inner = [at(2, 0, layer, shift) + half[layer] for layer in range(4)]
            return [inner[0]] + [inner[i] + half[i - 1] for i in (1, 2, 3)] + [half[3]]

        def along_y(layer, shift):
            v = at(3, 1, layer, shift)
            return at(2, 1, layer, shift) + 0.5 * (v + from_below(v))

        def along_z(layer):
            return at(2, 2, layer, 0) + 0.5 * (at(3, 2, layer, 0) + at(3, 2, layer, -1))

        tx = along_x(0)
        tx_next = along_x(1)
        ty = [along_y(layer, 0) for layer in range(4)]
        tz = [along_z(layer) for layer in range(4)]
        y_sum = [0.25 * (at(1, 1, layer, 0) + at(1, 1, layer, 1)) for layer in range(4)]
        z_own = [at(1, 2, layer, 0) for layer in range(4)]
        z_sum = [0.25 * (v + from_above(v)) for v in z_own]
        xs, ys, zs = [], [], []
        for layer in range(4):
            x_sum = at(1, 0, layer, 0) + at(1, 0, layer, 1)
            xs.append(
                at(0, 0, layer, 0) + 0.25 * (x_sum + from_above(x_sum))
                + (ty[layer] - along_y(layer, 1)) - (tz[layer] - from_above(tz[layer]))
            )
        for layer in range(-1, 5):
            y = z = None
            if layer >= 0:
                y = tx_next[layer] - tx[layer]
                z = tx[layer] - from_above(tx[layer])
            if 0 <= layer < 4:
                y = y + (at(0, 1, layer, 0) + y_sum[layer] + tz[layer])
                z = z + (at(0, 2, layer, 0) + z_sum[layer] - ty[layer])
            if layer < 3:
                y_more = y_sum[layer + 1] - tz[layer + 1]
                z_more = z_sum[layer + 1] + ty[layer + 1]
                y = y_more if y is None else y + y_more
                z = z_more if z is None else z + z_more
            ys.append(y)
            zs.append(z)
        for layer in range(2):
            out[0, layer, rows] = xs[layer + 1]
            out[1, layer, rows] = ys[layer + 2]
            out[2, layer, rows] = zs[layer + 2]
        up = (xs[3], ys[4], zs[4], ys[5], zs[5])
        down = (xs[0], ys[1], zs[1], ys[0], zs[0])
        for slot in range(5):
            sent[1 - odd, slot, rows] = up[slot]
            sent[odd, slot, rows] = down[slot]
    first[...] = sent[0]
    second[...] = sent[1]


def combine(place, part, first, second, mask, out, total):
    odd = place[1] % 2
    other = 1 - odd
    for comp in range(3):
        total[comp, odd] = part[comp, odd] + first[comp]
        total[comp, other] = part[comp, other] + second[comp]
    for comp in (1, 2):
        total[comp, odd] += second[comp + 2]
        total[comp, other] += first[comp + 2]
    for comp in range(3):
        for layer in range(2):
            out[comp, layer] = total[comp, layer].T * mask[comp, layer].astype(F32)


def local(residual, face_mask, conductivity, stencil):
    blocks = lax.axis_size("blk")

    def exchange(axis, first, second):
        size = lax.axis_size(axis)
        arrived = []
        for part, begin in ((first, 1), (second, 0)):
            pairs = [(i, i + 1) for i in range(begin, size - 1, 2)]
            pairs += [(j, i) for i, j in pairs]
            arrived.append(lax.ppermute(part, axis, pairs))
        return arrived

    place = jnp.stack(
        [lax.axis_index("grp"), lax.axis_index("blk"), jnp.int32(blocks - 1)]
    ).astype(jnp.int32)

    step = OMEGA / (stencil[:, 13] * np.eye(3, dtype=np.float32)).sum(2)
    table = step[:, None, :, None] * (CENTRE - stencil * step[:, None, None, :])
    table = jnp.broadcast_to(table.reshape(972, 1), (972, N))

    in_hbm = pl.BlockSpec(memory_space=pltpu.HBM)
    residual, mask, conductivity = (
        pltpu.with_memory_space_constraint(v, pltpu.HBM)
        for v in (residual, face_mask, conductivity)
    )
    own, first, second = call(
        mask_residual, "mask_residual",
        [(3, 2, N, N), (PLANES, N), (PLANES, N)],
        [smem(), in_hbm, in_hbm],
        [
            pltpu.VMEM((3, 2, N, N), F32),
            pltpu.VMEM((3, 2, N, N), jnp.int32),
            pltpu.VMEM((2, PLANES, N), F32),
            pltpu.SemaphoreType.DMA((2,)),
        ],
    )(place, residual, mask)
    z_first, z_second = exchange("grp", first, second)
    (chunks,) = call(
        invert, "invert", [(4, 2 * INV, N)], [in_hbm],
        [pltpu.VMEM((1, 2, N, 4 * N), F32), pltpu.SemaphoreType.DMA(())],
    )(conductivity)
    got = lax.all_to_all(chunks, "grp", split_axis=0, concat_axis=0, tiled=True)
    (weights,) = call(
        band, "band", [(4, 36 * 8, 2 * N)], [vmem()], dtype=BF16
    )(table)
    field, first, second = call(
        pack, "pack",
        [(2, 3, MROWS, N), (2, XROWS, N), (2, XROWS, N)],
        [smem()] + [vmem()] * 3,
        [pltpu.VMEM((2, PLANES, N), F32)],
    )(place, own, z_first, z_second)
    first, second = exchange("blk", first, second)
    part, first, second = call(
        correct, "correct",
        [(3, 2, N, N), (5, N, N), (5, N, N)],
        [smem()] + [vmem()] * 5,
        [
            pltpu.VMEM((2, 2, MROWS, N), F32),
            pltpu.VMEM((4, 3, 2, HROWS, N), F32),
            pltpu.VMEM((4, 3, 4, WROWS, N), F32),
            pltpu.VMEM((2, 5, N, N), F32),
        ],
    )(place, field, got, first, second, weights)
    first, second = exchange("blk", first, second)
    (out,) = call(
        combine, "combine", [(3, 2, N, N)], [smem()] + [vmem()] * 4,
        [pltpu.VMEM((3, 2, N, N), F32)],
    )(place, part, first, second, face_mask)
    return out


def solution(mesh):
    return jax.shard_map(
        local,
        mesh=mesh,
        in_specs=(
            P(None, "blk", None, "grp"),
            P(None, "blk", None, "grp"),
            P("grp", "blk", None, None),
            P(),
        ),
        out_specs=P(None, "blk", None, "grp"),
        check_vma=False,
    )
```

```python
import jax
import jax.numpy as jnp
import numpy as np
from jax import lax
from jax.experimental import pallas as pl
from jax.experimental.pallas import tpu as pltpu
from jax.sharding import PartitionSpec as P

OMEGA = 0.8
F32 = jnp.float32
BF16 = jnp.bfloat16
N = 128
INV = 136
PLANES = 32
MROWS = 144
HROWS = 144
WROWS = 136
BLOCK = 6
PAIRS = 11
TERM = 48
DEPTH = 3 * TERM
CENTRE = np.zeros((27, 3, 3), np.float32)
CENTRE[13] = 2.0 * np.eye(3)


def vmem():
    return pl.BlockSpec(memory_space=pltpu.VMEM)


def smem():
    return pl.BlockSpec(memory_space=pltpu.SMEM)


def call(kernel, name, out_shapes, in_specs, scratch=(), dtype=F32, outs=None):
    return pl.pallas_call(
        kernel,
        name=name,
        out_shape=[jax.ShapeDtypeStruct(shape, dtype) for shape in out_shapes],
        in_specs=in_specs,
        out_specs=[outs or vmem() for _ in out_shapes],
        scratch_shapes=list(scratch),
        compiler_params=pltpu.CompilerParams(vmem_limit_bytes=50 << 20),
    )


def from_below(v):
    lane = lax.broadcasted_iota(jnp.int32, v.shape, 1)
    return jnp.where(lane == 0, 0.0, pltpu.roll(v, 1, 1))


def from_above(v):
    lane = lax.broadcasted_iota(jnp.int32, v.shape, 1)
    return jnp.where(lane == N - 1, 0.0, pltpu.roll(v, N - 1, 1))


def mask_residual(place, res_hbm, mask_hbm, own, first, second, res, mask, sems):
    odd = place[1] % 2
    copies = [
        pltpu.make_async_copy(src, dst, sems.at[i])
        for i, (src, dst) in enumerate(((res_hbm, res), (mask_hbm, mask)))
    ]
    for copy in copies:
        copy.start()
    for copy in copies:
        copy.wait()
    for comp in range(3):
        for layer in range(2):
            own[comp, layer] = (res[comp, layer] * mask[comp, layer].astype(F32)).T
    for slot in range(2):
        first[slot] = own[slot + 1, odd]
        second[slot] = own[slot + 1, 1 - odd]


def invert(cond, after, chunks):
    for layer in range(2):
        base = layer * INV
        chunks[0, base : base + 2] = jnp.zeros((2, N), F32)
        chunks[3, base + 130 : base + 132] = jnp.zeros((2, N), F32)
        for j in range(4):
            v = (1.0 / cond[0, layer, :, j * N : (j + 1) * N]).T
            chunks[j, base + 2 : base + 130] = v
            chunks[j, base + 132 : base + INV] = jnp.zeros((4, N), F32)
            if j < 3:
                chunks[j + 1, base : base + 2] = v[N - 2 : N]
            if j > 0:
                chunks[j - 1, base + 130 : base + 132] = v[0:2]


def plane_row(comp, layer):
    if layer in (0, 1):
        return (comp * 2 + layer) * 3
    return 18 + ((comp - 1) * 2 + max(layer, 0) // 2) * 3


def pack(place, own, x_first, x_second, first, second, planes):
    z_odd = place[0] % 2
    odd = place[1] % 2

    def put(row, v):
        planes[0, row : row + 3] = v[0:3]
        planes[1, row : row + 3] = v[N - 3 : N]

    for comp in range(3):
        for layer in range(2):
            put(plane_row(comp, layer), own.at[comp, layer])
    for slot in range(2):
        low_row = plane_row(slot + 1, -1)
        for arrived, upper in ((x_first, odd), (x_second, 1 - odd)):
            row = low_row + 3 * upper
            v = arrived.at[slot]
            planes[0, pl.ds(row, 3)] = v[0:3]
            planes[1, pl.ds(row, 3)] = v[N - 3 : N]
    planes[:, 30:PLANES] = jnp.zeros((2, PLANES - 30, N), F32)
    first[...] = planes[z_odd]
    second[...] = planes[1 - z_odd]


def fill_masked(place, own, x_first, x_second, z_first, z_second, field, side, planes):
    z_odd = place[0] % 2
    odd = place[1] % 2
    planes[0] = z_first[...]
    planes[1] = z_second[...]
    for arrived, where in ((x_first, odd), (x_second, 1 - odd)):
        for slot in range(2):
            side[where, slot, 3 : 3 + N] = arrived[slot]

    def ends(ref, row):
        ref[0:3] = planes[z_odd, row : row + 3]
        ref[3 + N : 6 + N] = planes[1 - z_odd, row : row + 3]
        ref[6 + N : MROWS] = jnp.zeros((MROWS - N - 6, N), F32)

    for layer in range(2):
        for comp in range(3):
            field[layer, comp, 3 : 3 + N] = own[comp, layer]
            ends(field.at[layer, comp], plane_row(comp, layer))
    for where, layer in ((0, -1), (1, 2)):
        for slot in range(2):
            ends(side.at[where, slot], plane_row(slot + 1, layer))


def restrict_tile(field, side, place, start, rows):
    def at(layer, comp, shift):
        rows_at = slice(start + 1 + shift, start + 1 + shift + rows)
        if layer in (1, 2):
            return field[layer - 1, comp, rows_at]
        return side[layer // 3, comp - 1, rows_at]

    x0, xm, xp = (at(place, 0, s) for s in (0, -1, 1))
    y0, ym, yp = (at(place, 1, s) for s in (0, -1, 1))
    z0 = at(place, 2, 0)
    yl0, ylm, ylp = (at(place - 1, 1, s) for s in (0, -1, 1))
    zl0 = at(place - 1, 2, 0)
    yn0, ynm = (at(place + 1, 1, s) for s in (0, -1))
    zn0 = at(place + 1, 2, 0)
    xsum = x0 + xm
    zsum = z0 + zl0
    curl_x = z0 - from_below(z0) - y0 + ym
    curl_x_next = zn0 - from_below(zn0) - yn0 + ynm
    curl_y = x0 - xm - z0 + zl0
    curl_z = y0 - yl0 - x0 + from_below(x0)
    curl_z_next = yp - ylp - xp + from_below(xp)
    return (
        (x0, y0, z0),
        (
            0.25 * (xsum + from_below(xsum)),
            0.25 * (y0 + ym + (yl0 + ylm)),
            0.25 * (zsum + from_below(zsum)),
        ),
        (curl_x, curl_y, curl_z),
        (
            0.5 * (curl_x + curl_x_next),
            0.5 * (curl_y + from_above(curl_y)),
            0.5 * (curl_z + curl_z_next),
        ),
    )


def band(table, out):
    row = lax.broadcasted_iota(jnp.int32, (8, N), 0)
    lane = lax.broadcasted_iota(jnp.int32, (8, N), 1)

    def codes(at):
        term = (at >= TERM).astype(jnp.int32) + (at >= 2 * TERM).astype(jnp.int32)
        k = at - TERM * term
        dz = (k & 7) - row
        fits = (at < DEPTH) & (row < BLOCK) & (dz >= 0) & (dz < 3)
        return jnp.where(fits, (k >> 3) * 8 + dz, -1)

    code = (codes(lane), codes(lane + N))

    def fill(step, carry):
        space = step // 9
        entry = step % 9
        dy = entry // 3
        d = entry % 3
        rows = []
        for to in range(4):
            halves = [jnp.zeros((8, N), F32), jnp.zeros((8, N), F32)]
            for layer in range(2):
                dx = layer + 2 - to
                if dx < 0 or dx > 2:
                    continue
                for c in range(3):
                    for dz in range(3):
                        index = ((space * 27 + dx * 9 + dy * 3 + dz) * 3 + d) * 3 + c
                        value = table[pl.ds(index, 8, stride=0)]
                        for half in range(2 if c == 2 else 1):
                            hit = code[half] == (c * 2 + layer) * 8 + dz
                            halves[half] = jnp.where(hit, value, halves[half])
            parts = []
            for half, v in enumerate(halves):
                high = v.astype(BF16).astype(F32)
                parts.append(jnp.where(lane + half * N < 2 * TERM, high, v - high))
            rows.append(jnp.concatenate(parts, 1))
        start = pl.multiple_of(entry * 32, 32)
        out[space, pl.ds(start, 32)] = jnp.concatenate(rows, 0).astype(BF16)
        return carry

    lax.fori_loop(0, 36, fill, 0)


def correct(
    place, own, got, x_first, x_second, z_first, z_second, weights,
    out, first, second, field, side, planes, h, w, sent,
):
    grp = place[0]
    blk = place[1]
    odd = blk % 2
    fill_masked(place, own, x_first, x_second, z_first, z_second, field, side, planes)
    for layer in range(2):
        for tile in range(INV // 8):
            start = 8 * tile
            spaces = restrict_tile(field, side, layer + 1, start, 8)
            for space in range(4):
                row = layer * INV + start
                inv = got[space, row : row + 8]
                for comp in range(3):
                    h[space, comp, layer, start : start + 8] = spaces[space][comp] * inv

    def dense(space, carry):
        for pair in range(PAIRS):
            starts = (2 * BLOCK * pair, 2 * BLOCK * pair + BLOCK)
            fields = jnp.concatenate([
                jnp.concatenate(
                    [h[space, c, layer, at : at + 8] for c in range(3) for layer in range(2)], 0
                )
                for at in starts
            ], 1)
            high = fields.astype(BF16)
            low = (fields - high.astype(F32)).astype(BF16)
            sums = jnp.dot(
                weights[space, :, 0:DEPTH],
                jnp.concatenate([high, low, high], 0),
                preferred_element_type=F32,
            )
            for half, at in enumerate(starts):
                lanes = slice(half * N, half * N + N)
                for d in range(3):
                    for to in range(4):
                        below, here, above = (
                            sums[row * 8 : row * 8 + 8, lanes]
                            for row in ((dy * 3 + d) * 4 + to for dy in range(3))
                        )
                        w[space, d, to, at : at + 8] = here + (
                            from_below(below) + from_above(above)
                        )
        return carry

    lax.fori_loop(0, 4, dense, 0)

    def clear(layers, rows):
        for space in range(4):
            for d in range(3):
                for layer in layers:
                    w[space, d, layer, rows] = jnp.zeros((rows.stop - rows.start, N), F32)

    @pl.when(grp == 0)
    def _():
        clear(range(4), slice(0, 1))

    @pl.when(grp == 3)
    def _():
        clear(range(4), slice(N + 1, N + 2))

    @pl.when(blk == 0)
    def _():
        clear((0,), slice(0, WROWS))

    @pl.when(blk == place[2])
    def _():
        clear((3,), slice(0, WROWS))

    for tile in range(N // 8):
        start = 8 * tile
        rows = slice(start, start + 8)

        def at(space, d, layer, shift):
            return w[space, d, layer, start + 1 + shift : start + 9 + shift]

        def along_x(shift):
            half = [0.5 * at(3, 0, layer, shift) for layer in range(4)]
            inner = [at(2, 0, layer, shift) + half[layer] for layer in range(4)]
            return [inner[0]] + [inner[i] + half[i - 1] for i in (1, 2, 3)] + [half[3]]

        def along_y(layer, shift):
            v = at(3, 1, layer, shift)
            return at(2, 1, layer, shift) + 0.5 * (v + from_below(v))

        def along_z(layer):
            return at(2, 2, layer, 0) + 0.5 * (at(3, 2, layer, 0) + at(3, 2, layer, -1))

        tx = along_x(0)
        tx_next = along_x(1)
        ty = [along_y(layer, 0) for layer in range(4)]
        tz = [along_z(layer) for layer in range(4)]
        y_sum = [0.25 * (at(1, 1, layer, 0) + at(1, 1, layer, 1)) for layer in range(4)]
        z_own = [at(1, 2, layer, 0) for layer in range(4)]
        z_sum = [0.25 * (v + from_above(v)) for v in z_own]
        xs, ys, zs = [], [], []
        for layer in range(4):
            x_sum = at(1, 0, layer, 0) + at(1, 0, layer, 1)
            xs.append(
                at(0, 0, layer, 0) + 0.25 * (x_sum + from_above(x_sum))
                + (ty[layer] - along_y(layer, 1)) - (tz[layer] - from_above(tz[layer]))
            )
        for layer in range(-1, 5):
            y = z = None
            if layer >= 0:
                y = tx_next[layer] - tx[layer]
                z = tx[layer] - from_above(tx[layer])
            if 0 <= layer < 4:
                y = y + (at(0, 1, layer, 0) + y_sum[layer] + tz[layer])
                z = z + (at(0, 2, layer, 0) + z_sum[layer] - ty[layer])
            if layer < 3:
                y_more = y_sum[layer + 1] - tz[layer + 1]
                z_more = z_sum[layer + 1] + ty[layer + 1]
                y = y_more if y is None else y + y_more
                z = z_more if z is None else z + z_more
            ys.append(y)
            zs.append(z)
        for layer in range(2):
            out[0, layer, rows] = xs[layer + 1]
            out[1, layer, rows] = ys[layer + 2]
            out[2, layer, rows] = zs[layer + 2]
        up = (xs[3], ys[4], zs[4], ys[5], zs[5])
        down = (xs[0], ys[1], zs[1], ys[0], zs[0])
        for slot in range(5):
            sent[1 - odd, slot, rows] = up[slot]
            sent[odd, slot, rows] = down[slot]
    first[...] = sent[0]
    second[...] = sent[1]


def combine(place, part, first, second, mask, out_hbm, total, out, sems):
    odd = place[1] % 2
    other = 1 - odd
    copies = []
    for comp in range(3):
        at_odd = part[comp, odd] + first[comp]
        at_other = part[comp, other] + second[comp]
        if comp > 0:
            at_odd += second[comp + 2]
            at_other += first[comp + 2]
        total[comp, odd] = at_odd
        total[comp, other] = at_other
        for layer in range(2):
            out[comp, layer] = total[comp, layer].T * mask[comp, layer].astype(F32)
        copies.append(pltpu.make_async_copy(out.at[comp], out_hbm.at[comp], sems.at[comp]))
        copies[-1].start()
    for copy in copies:
        copy.wait()


def local(residual, face_mask, conductivity, stencil):
    blocks = lax.axis_size("blk")

    def exchange(axis, first, second):
        size = lax.axis_size(axis)
        arrived = []
        for part, begin in ((first, 1), (second, 0)):
            pairs = [(i, i + 1) for i in range(begin, size - 1, 2)]
            pairs += [(j, i) for i, j in pairs]
            arrived.append(lax.ppermute(part, axis, pairs))
        return arrived

    place = jnp.stack(
        [lax.axis_index("grp"), lax.axis_index("blk"), jnp.int32(blocks - 1)]
    ).astype(jnp.int32)

    step = OMEGA / (stencil[:, 13] * np.eye(3, dtype=np.float32)).sum(2)
    table = step[:, None, :, None] * (CENTRE - stencil * step[:, None, None, :])
    table = jnp.broadcast_to(table.reshape(972, 1), (972, N))

    in_hbm = pl.BlockSpec(memory_space=pltpu.HBM)
    residual, mask = (
        pltpu.with_memory_space_constraint(v, pltpu.HBM) for v in (residual, face_mask)
    )
    own, first, second = call(
        mask_residual, "mask_residual",
        [(3, 2, N, N), (2, N, N), (2, N, N)],
        [smem(), in_hbm, in_hbm],
        [
            pltpu.VMEM((3, 2, N, N), F32),
            pltpu.VMEM((3, 2, N, N), jnp.int32),
            pltpu.SemaphoreType.DMA((2,)),
        ],
    )(place, residual, mask)
    x_first, x_second = exchange("blk", first, second)
    (chunks,) = call(
        invert, "invert", [(4, 2 * INV, N)], [vmem(), pl.BlockSpec(memory_space=pl.ANY)]
    )(conductivity, first)
    got = lax.all_to_all(chunks, "grp", split_axis=0, concat_axis=0, tiled=True)
    first, second = call(
        pack, "pack", [(PLANES, N), (PLANES, N)], [smem()] + [vmem()] * 3,
        [pltpu.VMEM((2, PLANES, N), F32)],
    )(place, own, x_first, x_second)
    z_first, z_second = exchange("grp", first, second)
    (weights,) = call(
        band, "band", [(4, 36 * 8, 2 * N)], [vmem()], dtype=BF16
    )(table)
    part, first, second = call(
        correct, "correct",
        [(3, 2, N, N), (5, N, N), (5, N, N)],
        [smem()] + [vmem()] * 7,
        [
            pltpu.VMEM((2, 3, MROWS, N), F32),
            pltpu.VMEM((2, 2, MROWS, N), F32),
            pltpu.VMEM((2, PLANES, N), F32),
            pltpu.VMEM((4, 3, 2, HROWS, N), F32),
            pltpu.VMEM((4, 3, 4, WROWS, N), F32),
            pltpu.VMEM((2, 5, N, N), F32),
        ],
    )(place, own, got, x_first, x_second, z_first, z_second, weights)
    first, second = exchange("blk", first, second)
    (out,) = call(
        combine, "combine", [(3, 2, N, N)], [smem()] + [vmem()] * 4,
        [
            pltpu.VMEM((3, 2, N, N), F32),
            pltpu.VMEM((3, 2, N, N), F32),
            pltpu.SemaphoreType.DMA((3,)),
        ],
        outs=in_hbm,
    )(place, part, first, second, face_mask)
    return out


def solution(mesh):
    return jax.shard_map(
        local,
        mesh=mesh,
        in_specs=(
            P(None, "blk", None, "grp"),
            P(None, "blk", None, "grp"),
            P("grp", "blk", None, None),
            P(),
        ),
        out_specs=P(None, "blk", None, "grp"),
        check_vma=False,
    )
```

```python
import jax
import jax.numpy as jnp
from jax import lax
from jax.experimental import pallas as pl
from jax.experimental.pallas import tpu as pltpu
from jax.sharding import PartitionSpec as P

OMEGA = 0.8
F32 = jnp.float32
BF16 = jnp.bfloat16
N = 128
INV = 136
PLANES = 32
MROWS = 144
HROWS = 144
WROWS = 136
BLOCK = 6
PAIRS = 11
TERM = 48
DEPTH = 3 * TERM


def vmem():
    return pl.BlockSpec(memory_space=pltpu.VMEM)


def smem():
    return pl.BlockSpec(memory_space=pltpu.SMEM)


def call(kernel, name, out_shapes, in_specs, scratch=(), dtype=F32, outs=None):
    return pl.pallas_call(
        kernel,
        name=name,
        out_shape=[jax.ShapeDtypeStruct(shape, dtype) for shape in out_shapes],
        in_specs=in_specs,
        out_specs=[outs or vmem() for _ in out_shapes],
        scratch_shapes=list(scratch),
        compiler_params=pltpu.CompilerParams(vmem_limit_bytes=50 << 20),
    )


def from_below(v):
    lane = lax.broadcasted_iota(jnp.int32, v.shape, 1)
    return jnp.where(lane == 0, 0.0, pltpu.roll(v, 1, 1))


def from_above(v):
    lane = lax.broadcasted_iota(jnp.int32, v.shape, 1)
    return jnp.where(lane == N - 1, 0.0, pltpu.roll(v, N - 1, 1))


def mask_residual(place, res_hbm, mask_hbm, own, first, res, mask, sems):
    odd = place[1] % 2
    copies = [
        pltpu.make_async_copy(src, dst, sems.at[i])
        for i, (src, dst) in enumerate(((res_hbm, res), (mask_hbm, mask)))
    ]
    for copy in copies:
        copy.start()
    for copy in copies:
        copy.wait()
    for comp in range(3):
        for layer in range(2):
            own[comp, layer] = (res[comp, layer] * mask[comp, layer].astype(F32)).T
    for slot in range(2):
        first[slot] = own[slot + 1, odd]


def invert(place, cond, own, chunks, second):
    for slot in range(2):
        second[slot] = own[slot + 1, 1 - place[1] % 2]
    for layer in range(2):
        base = layer * INV
        chunks[0, base : base + 2] = jnp.zeros((2, N), F32)
        chunks[3, base + 130 : base + 132] = jnp.zeros((2, N), F32)
        for j in range(4):
            v = (1.0 / cond[0, layer, :, j * N : (j + 1) * N]).T
            chunks[j, base + 2 : base + 130] = v
            chunks[j, base + 132 : base + INV] = jnp.zeros((4, N), F32)
            if j < 3:
                chunks[j + 1, base : base + 2] = v[N - 2 : N]
            if j > 0:
                chunks[j - 1, base + 130 : base + 132] = v[0:2]


def plane_row(comp, layer):
    if layer in (0, 1):
        return (comp * 2 + layer) * 3
    return 18 + ((comp - 1) * 2 + max(layer, 0) // 2) * 3


def pack(place, own, x_first, x_second, first, second, planes):
    z_odd = place[0] % 2
    odd = place[1] % 2

    def put(row, v):
        planes[0, row : row + 3] = v[0:3]
        planes[1, row : row + 3] = v[N - 3 : N]

    for comp in range(3):
        for layer in range(2):
            put(plane_row(comp, layer), own.at[comp, layer])
    for slot in range(2):
        low_row = plane_row(slot + 1, -1)
        for arrived, upper in ((x_first, odd), (x_second, 1 - odd)):
            row = low_row + 3 * upper
            v = arrived.at[slot]
            planes[0, pl.ds(row, 3)] = v[0:3]
            planes[1, pl.ds(row, 3)] = v[N - 3 : N]
    planes[:, 30:PLANES] = jnp.zeros((2, PLANES - 30, N), F32)
    first[...] = planes[z_odd]
    second[...] = planes[1 - z_odd]


def fill_masked(place, own, x_first, x_second, z_first, z_second, field, side, planes):
    z_odd = place[0] % 2
    odd = place[1] % 2
    planes[0] = z_first[...]
    planes[1] = z_second[...]
    for arrived, where in ((x_first, odd), (x_second, 1 - odd)):
        for slot in range(2):
            side[where, slot, 3 : 3 + N] = arrived[slot]

    def ends(ref, row):
        ref[0:3] = planes[z_odd, row : row + 3]
        ref[3 + N : 6 + N] = planes[1 - z_odd, row : row + 3]
        ref[6 + N : MROWS] = jnp.zeros((MROWS - N - 6, N), F32)

    for layer in range(2):
        for comp in range(3):
            field[layer, comp, 3 : 3 + N] = own[comp, layer]
            ends(field.at[layer, comp], plane_row(comp, layer))
    for where, layer in ((0, -1), (1, 2)):
        for slot in range(2):
            ends(side.at[where, slot], plane_row(slot + 1, layer))


def restrict_tile(field, side, place, start, rows):
    def at(layer, comp, shift):
        rows_at = slice(start + 1 + shift, start + 1 + shift + rows)
        if layer in (1, 2):
            return field[layer - 1, comp, rows_at]
        return side[layer // 3, comp - 1, rows_at]

    x0, xm, xp = (at(place, 0, s) for s in (0, -1, 1))
    y0, ym, yp = (at(place, 1, s) for s in (0, -1, 1))
    z0 = at(place, 2, 0)
    yl0, ylm, ylp = (at(place - 1, 1, s) for s in (0, -1, 1))
    zl0 = at(place - 1, 2, 0)
    yn0, ynm = (at(place + 1, 1, s) for s in (0, -1))
    zn0 = at(place + 1, 2, 0)
    xsum = x0 + xm
    zsum = z0 + zl0
    curl_x = z0 - from_below(z0) - y0 + ym
    curl_x_next = zn0 - from_below(zn0) - yn0 + ynm
    curl_y = x0 - xm - z0 + zl0
    curl_z = y0 - yl0 - x0 + from_below(x0)
    curl_z_next = yp - ylp - xp + from_below(xp)
    return (
        (x0, y0, z0),
        (
            0.25 * (xsum + from_below(xsum)),
            0.25 * (y0 + ym + (yl0 + ylm)),
            0.25 * (zsum + from_below(zsum)),
        ),
        (curl_x, curl_y, curl_z),
        (
            0.5 * (curl_x + curl_x_next),
            0.5 * (curl_y + from_above(curl_y)),
            0.5 * (curl_z + curl_z_next),
        ),
    )


def band(table, out):
    row = lax.broadcasted_iota(jnp.int32, (8, N), 0)
    lane = lax.broadcasted_iota(jnp.int32, (8, N), 1)

    def codes(at):
        term = (at >= TERM).astype(jnp.int32) + (at >= 2 * TERM).astype(jnp.int32)
        k = at - TERM * term
        dz = (k & 7) - row
        fits = (at < DEPTH) & (row < BLOCK) & (dz >= 0) & (dz < 3)
        return jnp.where(fits, (k >> 3) * 8 + dz, -1)

    code = (codes(lane), codes(lane + N))

    def fill(step, carry):
        space = step // 9
        entry = step % 9
        dy = entry // 3
        d = entry % 3
        rows = []
        for to in range(4):
            halves = [jnp.zeros((8, N), F32), jnp.zeros((8, N), F32)]
            for layer in range(2):
                dx = layer + 2 - to
                if dx < 0 or dx > 2:
                    continue
                for c in range(3):
                    for dz in range(3):
                        index = ((space * 27 + dx * 9 + dy * 3 + dz) * 3 + d) * 3 + c
                        value = table[pl.ds(index, 8, stride=0)]
                        for half in range(2 if c == 2 else 1):
                            hit = code[half] == (c * 2 + layer) * 8 + dz
                            halves[half] = jnp.where(hit, value, halves[half])
            parts = []
            for half, v in enumerate(halves):
                high = v.astype(BF16).astype(F32)
                parts.append(jnp.where(lane + half * N < 2 * TERM, high, v - high))
            rows.append(jnp.concatenate(parts, 1))
        start = pl.multiple_of(entry * 32, 32)
        out[space, pl.ds(start, 32)] = jnp.concatenate(rows, 0).astype(BF16)
        return carry

    lax.fori_loop(0, 36, fill, 0)


def correct(
    place, own, got, x_first, x_second, z_first, z_second, weights,
    out, first, second, field, side, planes, h, w, sent,
):
    grp = place[0]
    blk = place[1]
    odd = blk % 2
    fill_masked(place, own, x_first, x_second, z_first, z_second, field, side, planes)
    for layer in range(2):
        for tile in range(INV // 8):
            start = 8 * tile
            spaces = restrict_tile(field, side, layer + 1, start, 8)
            for space in range(4):
                row = layer * INV + start
                inv = got[space, row : row + 8]
                for comp in range(3):
                    h[space, comp, layer, start : start + 8] = spaces[space][comp] * inv

    def dense(space, carry):
        for pair in range(PAIRS):
            starts = (2 * BLOCK * pair, 2 * BLOCK * pair + BLOCK)
            fields = jnp.concatenate([
                jnp.concatenate(
                    [h[space, c, layer, at : at + 8] for c in range(3) for layer in range(2)], 0
                )
                for at in starts
            ], 1)
            high = fields.astype(BF16)
            low = (fields - high.astype(F32)).astype(BF16)
            sums = jnp.dot(
                weights[space, :, 0:DEPTH],
                jnp.concatenate([high, low, high], 0),
                preferred_element_type=F32,
            )
            for half, at in enumerate(starts):
                lanes = slice(half * N, half * N + N)
                for d in range(3):
                    for to in range(4):
                        below, here, above = (
                            sums[row * 8 : row * 8 + 8, lanes]
                            for row in ((dy * 3 + d) * 4 + to for dy in range(3))
                        )
                        w[space, d, to, at : at + 8] = here + (
                            from_below(below) + from_above(above)
                        )
        return carry

    lax.fori_loop(0, 4, dense, 0)

    def clear(layers, rows):
        for space in range(4):
            for d in range(3):
                for layer in layers:
                    w[space, d, layer, rows] = jnp.zeros((rows.stop - rows.start, N), F32)

    @pl.when(grp == 0)
    def _():
        clear(range(4), slice(0, 1))

    @pl.when(grp == 3)
    def _():
        clear(range(4), slice(N + 1, N + 2))

    @pl.when(blk == 0)
    def _():
        clear((0,), slice(0, WROWS))

    @pl.when(blk == place[2])
    def _():
        clear((3,), slice(0, WROWS))

    for tile in range(N // 8):
        start = 8 * tile
        rows = slice(start, start + 8)

        def at(space, d, layer, shift):
            return w[space, d, layer, start + 1 + shift : start + 9 + shift]

        def along_x(shift):
            half = [0.5 * at(3, 0, layer, shift) for layer in range(4)]
            inner = [at(2, 0, layer, shift) + half[layer] for layer in range(4)]
            return [inner[0]] + [inner[i] + half[i - 1] for i in (1, 2, 3)] + [half[3]]

        def along_y(layer, shift):
            v = at(3, 1, layer, shift)
            return at(2, 1, layer, shift) + 0.5 * (v + from_below(v))

        def along_z(layer):
            return at(2, 2, layer, 0) + 0.5 * (at(3, 2, layer, 0) + at(3, 2, layer, -1))

        tx = along_x(0)
        tx_next = along_x(1)
        ty = [along_y(layer, 0) for layer in range(4)]
        tz = [along_z(layer) for layer in range(4)]
        y_sum = [0.25 * (at(1, 1, layer, 0) + at(1, 1, layer, 1)) for layer in range(4)]
        z_own = [at(1, 2, layer, 0) for layer in range(4)]
        z_sum = [0.25 * (v + from_above(v)) for v in z_own]
        xs, ys, zs = [], [], []
        for layer in range(4):
            x_sum = at(1, 0, layer, 0) + at(1, 0, layer, 1)
            xs.append(
                at(0, 0, layer, 0) + 0.25 * (x_sum + from_above(x_sum))
                + (ty[layer] - along_y(layer, 1)) - (tz[layer] - from_above(tz[layer]))
            )
        for layer in range(-1, 5):
            y = z = None
            if layer >= 0:
                y = tx_next[layer] - tx[layer]
                z = tx[layer] - from_above(tx[layer])
            if 0 <= layer < 4:
                y = y + (at(0, 1, layer, 0) + y_sum[layer] + tz[layer])
                z = z + (at(0, 2, layer, 0) + z_sum[layer] - ty[layer])
            if layer < 3:
                y_more = y_sum[layer + 1] - tz[layer + 1]
                z_more = z_sum[layer + 1] + ty[layer + 1]
                y = y_more if y is None else y + y_more
                z = z_more if z is None else z + z_more
            ys.append(y)
            zs.append(z)
        for layer in range(2):
            out[0, layer, rows] = xs[layer + 1]
            out[1, layer, rows] = ys[layer + 2]
            out[2, layer, rows] = zs[layer + 2]
        up = (xs[3], ys[4], zs[4], ys[5], zs[5])
        down = (xs[0], ys[1], zs[1], ys[0], zs[0])
        for slot in range(5):
            sent[1 - odd, slot, rows] = up[slot]
            sent[odd, slot, rows] = down[slot]
    first[...] = sent[0]
    second[...] = sent[1]


def combine(place, part, first, second, mask, out_hbm, total, out, sems):
    odd = place[1] % 2
    other = 1 - odd
    copies = []
    for comp in range(3):
        at_odd = part[comp, odd] + first[comp]
        at_other = part[comp, other] + second[comp]
        if comp > 0:
            at_odd += second[comp + 2]
            at_other += first[comp + 2]
        total[comp, odd] = at_odd
        total[comp, other] = at_other
        for layer in range(2):
            out[comp, layer] = total[comp, layer].T * mask[comp, layer].astype(F32)
        copies.append(pltpu.make_async_copy(out.at[comp], out_hbm.at[comp], sems.at[comp]))
        copies[-1].start()
    for copy in copies:
        copy.wait()


def local(residual, face_mask, conductivity, stencil):
    blocks = lax.axis_size("blk")

    def swap(axis, message, begin):
        pairs = [(i, i + 1) for i in range(begin, lax.axis_size(axis) - 1, 2)]
        return lax.ppermute(message, axis, pairs + [(j, i) for i, j in pairs])

    def exchange(axis, first, second):
        return swap(axis, first, 1), swap(axis, second, 0)

    place = jnp.stack(
        [lax.axis_index("grp"), lax.axis_index("blk"), jnp.int32(blocks - 1)]
    ).astype(jnp.int32)

    at = [lax.broadcasted_iota(jnp.int32, stencil.shape, dim) for dim in range(4)]
    diagonal = at[2] == at[3]
    centre = jnp.where(diagonal[:, 13], stencil[:, 13], 0.0)
    step = OMEGA / centre.sum(2)
    twice = jnp.where(diagonal & (at[1] == 13), 2.0, 0.0)
    table = step[:, None, :, None] * (twice - stencil * step[:, None, None, :])
    table = jnp.broadcast_to(table.reshape(972, 1), (972, N))

    in_hbm = pl.BlockSpec(memory_space=pltpu.HBM)
    residual, mask = (
        pltpu.with_memory_space_constraint(v, pltpu.HBM) for v in (residual, face_mask)
    )
    own, first = call(
        mask_residual, "mask_residual",
        [(3, 2, N, N), (2, N, N)],
        [smem(), in_hbm, in_hbm],
        [
            pltpu.VMEM((3, 2, N, N), F32),
            pltpu.VMEM((3, 2, N, N), jnp.int32),
            pltpu.SemaphoreType.DMA((2,)),
        ],
    )(place, residual, mask)
    x_first = swap("blk", first, 1)
    chunks, second = call(
        invert, "invert", [(4, 2 * INV, N), (2, N, N)], [smem()] + [vmem()] * 2
    )(place, conductivity, own)
    x_second = swap("blk", second, 0)
    got = lax.all_to_all(chunks, "grp", split_axis=0, concat_axis=0, tiled=True)
    first, second = call(
        pack, "pack", [(PLANES, N), (PLANES, N)], [smem()] + [vmem()] * 3,
        [pltpu.VMEM((2, PLANES, N), F32)],
    )(place, own, x_first, x_second)
    z_first, z_second = exchange("grp", first, second)
    (weights,) = call(
        band, "band", [(4, 36 * 8, 2 * N)], [vmem()], dtype=BF16
    )(table)
    part, first, second = call(
        correct, "correct",
        [(3, 2, N, N), (5, N, N), (5, N, N)],
        [smem()] + [vmem()] * 7,
        [
            pltpu.VMEM((2, 3, MROWS, N), F32),
            pltpu.VMEM((2, 2, MROWS, N), F32),
            pltpu.VMEM((2, PLANES, N), F32),
            pltpu.VMEM((4, 3, 2, HROWS, N), F32),
            pltpu.VMEM((4, 3, 4, WROWS, N), F32),
            pltpu.VMEM((2, 5, N, N), F32),
        ],
    )(place, own, got, x_first, x_second, z_first, z_second, weights)
    first, second = exchange("blk", first, second)
    (out,) = call(
        combine, "combine", [(3, 2, N, N)], [smem()] + [vmem()] * 4,
        [
            pltpu.VMEM((3, 2, N, N), F32),
            pltpu.VMEM((3, 2, N, N), F32),
            pltpu.SemaphoreType.DMA((3,)),
        ],
        outs=in_hbm,
    )(place, part, first, second, face_mask)
    return out


def solution(mesh):
    return jax.shard_map(
        local,
        mesh=mesh,
        in_specs=(
            P(None, "blk", None, "grp"),
            P(None, "blk", None, "grp"),
            P("grp", "blk", None, None),
            P(),
        ),
        out_specs=P(None, "blk", None, "grp"),
        check_vma=False,
    )
```

```python
import jax
import jax.numpy as jnp
from jax import lax
from jax.experimental import pallas as pl
from jax.experimental.pallas import tpu as pltpu
from jax.sharding import PartitionSpec as P

OMEGA = 0.8
F32 = jnp.float32
BF16 = jnp.bfloat16
N = 128
INV = 136
PLANES = 32
MROWS = 144
HROWS = 136
WROWS = 136
BLOCK = 6
PAIRS = 11
TERM = 48
DEPTH = 3 * TERM


def vmem():
    return pl.BlockSpec(memory_space=pltpu.VMEM)


def smem():
    return pl.BlockSpec(memory_space=pltpu.SMEM)


def call(kernel, out_shapes, in_specs, scratch=(), dtype=F32, outs=None):
    return pl.pallas_call(
        kernel,
        out_shape=[jax.ShapeDtypeStruct(shape, dtype) for shape in out_shapes],
        in_specs=in_specs,
        out_specs=[outs or vmem() for _ in out_shapes],
        scratch_shapes=list(scratch),
        compiler_params=pltpu.CompilerParams(vmem_limit_bytes=50 << 20),
    )


def from_below(v):
    lane = lax.broadcasted_iota(jnp.int32, v.shape, 1)
    return jnp.where(lane == 0, 0.0, pltpu.roll(v, 1, 1))


def from_above(v):
    lane = lax.broadcasted_iota(jnp.int32, v.shape, 1)
    return jnp.where(lane == N - 1, 0.0, pltpu.roll(v, N - 1, 1))


def mask_residual(
    place, res_hbm, mask_hbm, cond_hbm, own, first, second, cond, res, mask, sems
):
    odd = place[1] % 2
    copies = [
        pltpu.make_async_copy(src, dst, sems.at[i])
        for i, (src, dst) in enumerate(((res_hbm, res), (mask_hbm, mask), (cond_hbm, cond)))
    ]
    for copy in copies:
        copy.start()
    copies[0].wait()
    copies[1].wait()
    for comp in range(3):
        for layer in range(2):
            own[comp, layer] = (res[comp, layer] * mask[comp, layer].astype(F32)).T
    for slot in range(2):
        first[slot] = own[slot + 1, odd]
        second[slot] = own[slot + 1, 1 - odd]
    copies[2].wait()


def invert(cond, chunks):
    for layer in range(2):
        base = layer * INV
        chunks[0, base : base + 2] = jnp.zeros((2, N), F32)
        chunks[3, base + 130 : base + 132] = jnp.zeros((2, N), F32)
        for j in range(4):
            v = (1.0 / cond[0, layer, :, j * N : (j + 1) * N]).T
            chunks[j, base + 2 : base + 130] = v
            chunks[j, base + 132 : base + INV] = jnp.zeros((4, N), F32)
            if j < 3:
                chunks[j + 1, base : base + 2] = v[N - 2 : N]
            if j > 0:
                chunks[j - 1, base + 130 : base + 132] = v[0:2]


def plane_row(comp, layer):
    if layer in (0, 1):
        return (comp * 2 + layer) * 3
    return 18 + ((comp - 1) * 2 + max(layer, 0) // 2) * 3


def pack(place, own, x_first, x_second, first, second, planes):
    z_odd = place[0] % 2
    odd = place[1] % 2

    def put(row, v):
        planes[0, row : row + 3] = v[0:3]
        planes[1, row : row + 3] = v[N - 3 : N]

    for comp in range(3):
        for layer in range(2):
            put(plane_row(comp, layer), own.at[comp, layer])
    for slot in range(2):
        low_row = plane_row(slot + 1, -1)
        for arrived, upper in ((x_first, odd), (x_second, 1 - odd)):
            row = low_row + 3 * upper
            v = arrived.at[slot]
            planes[0, pl.ds(row, 3)] = v[0:3]
            planes[1, pl.ds(row, 3)] = v[N - 3 : N]
    planes[:, 30:PLANES] = jnp.zeros((2, PLANES - 30, N), F32)
    first[...] = planes[z_odd]
    second[...] = planes[1 - z_odd]


def fill_masked(place, own, x_first, x_second, z_first, z_second, field, side, planes):
    z_odd = place[0] % 2
    odd = place[1] % 2
    planes[0] = z_first[...]
    planes[1] = z_second[...]
    for arrived, where in ((x_first, odd), (x_second, 1 - odd)):
        for slot in range(2):
            side[where, slot, 3 : 3 + N] = arrived[slot]

    def ends(ref, row):
        ref[0:3] = planes[z_odd, row : row + 3]
        ref[3 + N : 6 + N] = planes[1 - z_odd, row : row + 3]
        ref[6 + N : MROWS] = jnp.zeros((MROWS - N - 6, N), F32)

    for layer in range(2):
        for comp in range(3):
            field[layer, comp, 3 : 3 + N] = own[comp, layer]
            ends(field.at[layer, comp], plane_row(comp, layer))
    for where, layer in ((0, -1), (1, 2)):
        for slot in range(2):
            ends(side.at[where, slot], plane_row(slot + 1, layer))


def restrict_tile(field, side, place, start, rows):
    def at(layer, comp, shift):
        rows_at = slice(start + 1 + shift, start + 1 + shift + rows)
        if layer in (1, 2):
            return field[layer - 1, comp, rows_at]
        return side[layer // 3, comp - 1, rows_at]

    x0, xm, xp = (at(place, 0, s) for s in (0, -1, 1))
    y0, ym, yp = (at(place, 1, s) for s in (0, -1, 1))
    z0 = at(place, 2, 0)
    yl0, ylm, ylp = (at(place - 1, 1, s) for s in (0, -1, 1))
    zl0 = at(place - 1, 2, 0)
    yn0, ynm = (at(place + 1, 1, s) for s in (0, -1))
    zn0 = at(place + 1, 2, 0)
    xsum = x0 + xm
    zsum = z0 + zl0
    curl_x = z0 - from_below(z0) - y0 + ym
    curl_x_next = zn0 - from_below(zn0) - yn0 + ynm
    curl_y = x0 - xm - z0 + zl0
    curl_z = y0 - yl0 - x0 + from_below(x0)
    curl_z_next = yp - ylp - xp + from_below(xp)
    return (
        (x0, y0, z0),
        (
            0.25 * (xsum + from_below(xsum)),
            0.25 * (y0 + ym + (yl0 + ylm)),
            0.25 * (zsum + from_below(zsum)),
        ),
        (curl_x, curl_y, curl_z),
        (
            0.5 * (curl_x + curl_x_next),
            0.5 * (curl_y + from_above(curl_y)),
            0.5 * (curl_z + curl_z_next),
        ),
    )


def restrict(
    place, own, x_first, x_second, z_first, z_second, restricted, field, side, planes
):
    fill_masked(place, own, x_first, x_second, z_first, z_second, field, side, planes)
    for layer in range(2):
        for tile in range(HROWS // 8):
            start = 8 * tile
            spaces = restrict_tile(field, side, layer + 1, start, 8)
            for space in range(4):
                for comp in range(3):
                    restricted[space, comp, layer, start : start + 8] = spaces[space][comp]


def band(table, out):
    row = lax.broadcasted_iota(jnp.int32, (8, N), 0)
    lane = lax.broadcasted_iota(jnp.int32, (8, N), 1)

    def codes(at):
        term = (at >= TERM).astype(jnp.int32) + (at >= 2 * TERM).astype(jnp.int32)
        k = at - TERM * term
        dz = (k & 7) - row
        fits = (at < DEPTH) & (row < BLOCK) & (dz >= 0) & (dz < 3)
        return jnp.where(fits, (k >> 3) * 8 + dz, -1)

    code = (codes(lane), codes(lane + N))

    def fill(step, carry):
        space = step // 9
        entry = step % 9
        dy = entry // 3
        d = entry % 3
        rows = []
        for to in range(4):
            halves = [jnp.zeros((8, N), F32), jnp.zeros((8, N), F32)]
            for layer in range(2):
                dx = layer + 2 - to
                if dx < 0 or dx > 2:
                    continue
                for c in range(3):
                    for dz in range(3):
                        index = ((space * 27 + dx * 9 + dy * 3 + dz) * 3 + d) * 3 + c
                        value = table[pl.ds(index, 8, stride=0)]
                        for half in range(2 if c == 2 else 1):
                            hit = code[half] == (c * 2 + layer) * 8 + dz
                            halves[half] = jnp.where(hit, value, halves[half])
            parts = []
            for half, v in enumerate(halves):
                high = v.astype(BF16).astype(F32)
                parts.append(jnp.where(lane + half * N < 2 * TERM, high, v - high))
            rows.append(jnp.concatenate(parts, 1))
        start = pl.multiple_of(entry * 32, 32)
        out[space, pl.ds(start, 32)] = jnp.concatenate(rows, 0).astype(BF16)
        return carry

    lax.fori_loop(0, 36, fill, 0)


def correct(place, restricted, got, weights, out, first, second, w, sent):
    grp = place[0]
    blk = place[1]
    odd = blk % 2

    def dense(space, carry):
        for pair in range(PAIRS):
            starts = (2 * BLOCK * pair, 2 * BLOCK * pair + BLOCK)
            blocks = []
            for at in starts:
                inv = [got[space, layer * INV + at : layer * INV + at + 8] for layer in range(2)]
                blocks.append(jnp.concatenate([
                    restricted[space, c, layer, at : at + 8] * inv[layer]
                    for c in range(3) for layer in range(2)
                ], 0))
            fields = jnp.concatenate(blocks, 1)
            high = fields.astype(BF16)
            low = (fields - high.astype(F32)).astype(BF16)
            sums = jnp.dot(
                weights[space, :, 0:DEPTH],
                jnp.concatenate([high, low, high], 0),
                preferred_element_type=F32,
            )
            for half, at in enumerate(starts):
                lanes = slice(half * N, half * N + N)
                for d in range(3):
                    for to in range(4):
                        below, here, above = (
                            sums[row * 8 : row * 8 + 8, lanes]
                            for row in ((dy * 3 + d) * 4 + to for dy in range(3))
                        )
                        w[space, d, to, at : at + 8] = here + (
                            from_below(below) + from_above(above)
                        )
        return carry

    lax.fori_loop(0, 4, dense, 0)

    def clear(layers, rows):
        for space in range(4):
            for d in range(3):
                for layer in layers:
                    w[space, d, layer, rows] = jnp.zeros((rows.stop - rows.start, N), F32)

    @pl.when(grp == 0)
    def _():
        clear(range(4), slice(0, 1))

    @pl.when(grp == 3)
    def _():
        clear(range(4), slice(N + 1, N + 2))

    @pl.when(blk == 0)
    def _():
        clear((0,), slice(0, WROWS))

    @pl.when(blk == place[2])
    def _():
        clear((3,), slice(0, WROWS))

    for tile in range(N // 8):
        start = 8 * tile
        rows = slice(start, start + 8)

        def at(space, d, layer, shift):
            return w[space, d, layer, start + 1 + shift : start + 9 + shift]

        def along_x(shift):
            half = [0.5 * at(3, 0, layer, shift) for layer in range(4)]
            inner = [at(2, 0, layer, shift) + half[layer] for layer in range(4)]
            return [inner[0]] + [inner[i] + half[i - 1] for i in (1, 2, 3)] + [half[3]]

        def along_y(layer, shift):
            v = at(3, 1, layer, shift)
            return at(2, 1, layer, shift) + 0.5 * (v + from_below(v))

        def along_z(layer):
            return at(2, 2, layer, 0) + 0.5 * (at(3, 2, layer, 0) + at(3, 2, layer, -1))

        tx = along_x(0)
        tx_next = along_x(1)
        ty = [along_y(layer, 0) for layer in range(4)]
        tz = [along_z(layer) for layer in range(4)]
        y_sum = [0.25 * (at(1, 1, layer, 0) + at(1, 1, layer, 1)) for layer in range(4)]
        z_own = [at(1, 2, layer, 0) for layer in range(4)]
        z_sum = [0.25 * (v + from_above(v)) for v in z_own]
        xs, ys, zs = [], [], []
        for layer in range(4):
            x_sum = at(1, 0, layer, 0) + at(1, 0, layer, 1)
            xs.append(
                at(0, 0, layer, 0) + 0.25 * (x_sum + from_above(x_sum))
                + (ty[layer] - along_y(layer, 1)) - (tz[layer] - from_above(tz[layer]))
            )
        for layer in range(-1, 5):
            y = z = None
            if layer >= 0:
                y = tx_next[layer] - tx[layer]
                z = tx[layer] - from_above(tx[layer])
            if 0 <= layer < 4:
                y = y + (at(0, 1, layer, 0) + y_sum[layer] + tz[layer])
                z = z + (at(0, 2, layer, 0) + z_sum[layer] - ty[layer])
            if layer < 3:
                y_more = y_sum[layer + 1] - tz[layer + 1]
                z_more = z_sum[layer + 1] + ty[layer + 1]
                y = y_more if y is None else y + y_more
                z = z_more if z is None else z + z_more
            ys.append(y)
            zs.append(z)
        for layer in range(2):
            out[0, layer, rows] = xs[layer + 1]
            out[1, layer, rows] = ys[layer + 2]
            out[2, layer, rows] = zs[layer + 2]
        up = (xs[3], ys[4], zs[4], ys[5], zs[5])
        down = (xs[0], ys[1], zs[1], ys[0], zs[0])
        for slot in range(5):
            sent[1 - odd, slot, rows] = up[slot]
            sent[odd, slot, rows] = down[slot]
    first[...] = sent[0]
    second[...] = sent[1]


def combine(place, part, first, second, mask, out_hbm, total, out, sems):
    odd = place[1] % 2
    other = 1 - odd
    copies = []
    for comp in range(3):
        at_odd = part[comp, odd] + first[comp]
        at_other = part[comp, other] + second[comp]
        if comp > 0:
            at_odd += second[comp + 2]
            at_other += first[comp + 2]
        total[comp, odd] = at_odd
        total[comp, other] = at_other
        for layer in range(2):
            out[comp, layer] = total[comp, layer].T * mask[comp, layer].astype(F32)
        copies.append(pltpu.make_async_copy(out.at[comp], out_hbm.at[comp], sems.at[comp]))
        copies[-1].start()
    for copy in copies:
        copy.wait()


def correction(residual, face_mask, conductivity, stencil):
    blocks = lax.axis_size("blk")

    def swap(axis, message, begin):
        pairs = [(i, i + 1) for i in range(begin, lax.axis_size(axis) - 1, 2)]
        return lax.ppermute(message, axis, pairs + [(j, i) for i, j in pairs])

    def exchange(axis, first, second):
        return swap(axis, first, 1), swap(axis, second, 0)

    place = jnp.stack(
        [lax.axis_index("grp"), lax.axis_index("blk"), jnp.int32(blocks - 1)]
    ).astype(jnp.int32)

    at = [lax.broadcasted_iota(jnp.int32, stencil.shape, dim) for dim in range(4)]
    diagonal = at[2] == at[3]
    centre = jnp.where(diagonal[:, 13], stencil[:, 13], 0.0)
    step = OMEGA / centre.sum(2)
    twice = jnp.where(diagonal & (at[1] == 13), 2.0, 0.0)
    table = step[:, None, :, None] * (twice - stencil * step[:, None, None, :])
    table = jnp.broadcast_to(table.reshape(972, 1), (972, N))

    in_hbm = pl.BlockSpec(memory_space=pltpu.HBM)
    residual, mask, conductivity = (
        pltpu.with_memory_space_constraint(v, pltpu.HBM)
        for v in (residual, face_mask, conductivity)
    )
    own, first, second, cond = call(
        mask_residual,
        [(3, 2, N, N), (2, N, N), (2, N, N), (1, 2, N, 4 * N)],
        [smem()] + [in_hbm] * 3,
        [
            pltpu.VMEM((3, 2, N, N), F32),
            pltpu.VMEM((3, 2, N, N), jnp.int32),
            pltpu.SemaphoreType.DMA((3,)),
        ],
    )(place, residual, mask, conductivity)
    x_first = swap("blk", first, 1)
    x_second = swap("blk", second, 0)
    (chunks,) = call(invert, [(4, 2 * INV, N)], [vmem()])(cond)
    got = lax.all_to_all(chunks, "grp", split_axis=0, concat_axis=0, tiled=True)
    first, second = call(
        pack, [(PLANES, N), (PLANES, N)], [smem()] + [vmem()] * 3,
        [pltpu.VMEM((2, PLANES, N), F32)],
    )(place, own, x_first, x_second)
    z_first, z_second = exchange("grp", first, second)
    (weights,) = call(band, [(4, 36 * 8, 2 * N)], [vmem()], dtype=BF16)(table)
    (restricted,) = call(
        restrict, [(4, 3, 2, HROWS, N)], [smem()] + [vmem()] * 5,
        [
            pltpu.VMEM((2, 3, MROWS, N), F32),
            pltpu.VMEM((2, 2, MROWS, N), F32),
            pltpu.VMEM((2, PLANES, N), F32),
        ],
    )(place, own, x_first, x_second, z_first, z_second)
    part, first, second = call(
        correct,
        [(3, 2, N, N), (5, N, N), (5, N, N)],
        [smem()] + [vmem()] * 3,
        [
            pltpu.VMEM((4, 3, 4, WROWS, N), F32),
            pltpu.VMEM((2, 5, N, N), F32),
        ],
    )(place, restricted, got, weights)
    first, second = exchange("blk", first, second)
    (out,) = call(
        combine, [(3, 2, N, N)], [smem()] + [vmem()] * 4,
        [
            pltpu.VMEM((3, 2, N, N), F32),
            pltpu.VMEM((3, 2, N, N), F32),
            pltpu.SemaphoreType.DMA((3,)),
        ],
        outs=in_hbm,
    )(place, part, first, second, face_mask)
    return out


def solution(mesh):
    return jax.shard_map(
        correction,
        mesh=mesh,
        in_specs=(
            P(None, "blk", None, "grp"),
            P(None, "blk", None, "grp"),
            P("grp", "blk", None, None),
            P(),
        ),
        out_specs=P(None, "blk", None, "grp"),
        check_vma=False,
    )
```

```python
import jax
import jax.numpy as jnp
from jax import lax
from jax.experimental import pallas as pl
from jax.experimental.pallas import tpu as pltpu
from jax.sharding import PartitionSpec as P

OMEGA = 0.8
F32 = jnp.float32
BF16 = jnp.bfloat16
N = 128
INV = 136
PLANES = 32
MROWS = 144
HROWS = 136
WROWS = 136
BLOCK = 6
PAIRS = 11
TERM = 48
DEPTH = 3 * TERM


def vmem():
    return pl.BlockSpec(memory_space=pltpu.VMEM)


def smem():
    return pl.BlockSpec(memory_space=pltpu.SMEM)


def call(kernel, out_shapes, in_specs, scratch=(), dtype=F32, outs=None):
    return pl.pallas_call(
        kernel,
        out_shape=[jax.ShapeDtypeStruct(shape, dtype) for shape in out_shapes],
        in_specs=in_specs,
        out_specs=[outs or vmem() for _ in out_shapes],
        scratch_shapes=list(scratch),
        compiler_params=pltpu.CompilerParams(vmem_limit_bytes=50 << 20),
    )


def from_below(v):
    lane = lax.broadcasted_iota(jnp.int32, v.shape, 1)
    return jnp.where(lane == 0, 0.0, pltpu.roll(v, 1, 1))


def from_above(v):
    lane = lax.broadcasted_iota(jnp.int32, v.shape, 1)
    return jnp.where(lane == N - 1, 0.0, pltpu.roll(v, N - 1, 1))


def mask_residual(
    place, res_hbm, mask_hbm, cond_hbm, own, first, second, chunks, cond, res, mask, sems
):
    odd = place[1] % 2
    copies = [
        pltpu.make_async_copy(src, dst, sems.at[i])
        for i, (src, dst) in enumerate(((res_hbm, res), (mask_hbm, mask), (cond_hbm, cond)))
    ]
    for copy in copies:
        copy.start()
    copies[0].wait()
    copies[1].wait()
    for comp in range(3):
        for layer in range(2):
            own[comp, layer] = (res[comp, layer] * mask[comp, layer].astype(F32)).T
    for slot in range(2):
        first[slot] = own[slot + 1, odd]
        second[slot] = own[slot + 1, 1 - odd]
    copies[2].wait()
    invert(cond, chunks)


def invert(cond, chunks):
    for layer in range(2):
        base = layer * INV
        chunks[0, base : base + 2] = jnp.zeros((2, N), F32)
        chunks[3, base + 130 : base + 132] = jnp.zeros((2, N), F32)
        for j in range(4):
            v = (1.0 / cond[0, layer, :, j * N : (j + 1) * N]).T
            chunks[j, base + 2 : base + 130] = v
            chunks[j, base + 132 : base + INV] = jnp.zeros((4, N), F32)
            if j < 3:
                chunks[j + 1, base : base + 2] = v[N - 2 : N]
            if j > 0:
                chunks[j - 1, base + 130 : base + 132] = v[0:2]


def plane_row(comp, layer):
    if layer in (0, 1):
        return (comp * 2 + layer) * 3
    return 18 + ((comp - 1) * 2 + max(layer, 0) // 2) * 3


def pack(place, own, x_first, x_second, weights, first, second, planes):
    z_odd = place[0] % 2
    odd = place[1] % 2

    def put(row, v):
        planes[0, row : row + 3] = v[0:3]
        planes[1, row : row + 3] = v[N - 3 : N]

    for comp in range(3):
        for layer in range(2):
            put(plane_row(comp, layer), own.at[comp, layer])
    for slot in range(2):
        low_row = plane_row(slot + 1, -1)
        for arrived, upper in ((x_first, odd), (x_second, 1 - odd)):
            row = low_row + 3 * upper
            v = arrived.at[slot]
            planes[0, pl.ds(row, 3)] = v[0:3]
            planes[1, pl.ds(row, 3)] = v[N - 3 : N]
    planes[:, 30:PLANES] = jnp.zeros((2, PLANES - 30, N), F32)
    first[...] = planes[z_odd]
    second[...] = planes[1 - z_odd]


def fill_masked(place, own, x_first, x_second, z_first, z_second, field, side, planes):
    z_odd = place[0] % 2
    odd = place[1] % 2
    planes[0] = z_first[...]
    planes[1] = z_second[...]
    for arrived, where in ((x_first, odd), (x_second, 1 - odd)):
        for slot in range(2):
            side[where, slot, 3 : 3 + N] = arrived[slot]

    def ends(ref, row):
        ref[0:3] = planes[z_odd, row : row + 3]
        ref[3 + N : 6 + N] = planes[1 - z_odd, row : row + 3]
        ref[6 + N : MROWS] = jnp.zeros((MROWS - N - 6, N), F32)

    for layer in range(2):
        for comp in range(3):
            field[layer, comp, 3 : 3 + N] = own[comp, layer]
            ends(field.at[layer, comp], plane_row(comp, layer))
    for where, layer in ((0, -1), (1, 2)):
        for slot in range(2):
            ends(side.at[where, slot], plane_row(slot + 1, layer))


def restrict_tile(field, side, place, start, rows):
    def at(layer, comp, shift):
        rows_at = slice(start + 1 + shift, start + 1 + shift + rows)
        if layer in (1, 2):
            return field[layer - 1, comp, rows_at]
        return side[layer // 3, comp - 1, rows_at]

    x0, xm, xp = (at(place, 0, s) for s in (0, -1, 1))
    y0, ym, yp = (at(place, 1, s) for s in (0, -1, 1))
    z0 = at(place, 2, 0)
    yl0, ylm, ylp = (at(place - 1, 1, s) for s in (0, -1, 1))
    zl0 = at(place - 1, 2, 0)
    yn0, ynm = (at(place + 1, 1, s) for s in (0, -1))
    zn0 = at(place + 1, 2, 0)
    xsum = x0 + xm
    zsum = z0 + zl0
    curl_x = z0 - from_below(z0) - y0 + ym
    curl_x_next = zn0 - from_below(zn0) - yn0 + ynm
    curl_y = x0 - xm - z0 + zl0
    curl_z = y0 - yl0 - x0 + from_below(x0)
    curl_z_next = yp - ylp - xp + from_below(xp)
    return (
        (x0, y0, z0),
        (
            0.25 * (xsum + from_below(xsum)),
            0.25 * (y0 + ym + (yl0 + ylm)),
            0.25 * (zsum + from_below(zsum)),
        ),
        (curl_x, curl_y, curl_z),
        (
            0.5 * (curl_x + curl_x_next),
            0.5 * (curl_y + from_above(curl_y)),
            0.5 * (curl_z + curl_z_next),
        ),
    )


def restrict(
    place, own, x_first, x_second, z_first, z_second, restricted, field, side, planes
):
    fill_masked(place, own, x_first, x_second, z_first, z_second, field, side, planes)
    for layer in range(2):
        for tile in range(HROWS // 8):
            start = 8 * tile
            spaces = restrict_tile(field, side, layer + 1, start, 8)
            for space in range(4):
                for comp in range(3):
                    restricted[space, comp, layer, start : start + 8] = spaces[space][comp]


def band(table, out):
    row = lax.broadcasted_iota(jnp.int32, (8, N), 0)
    lane = lax.broadcasted_iota(jnp.int32, (8, N), 1)

    def codes(at):
        term = (at >= TERM).astype(jnp.int32) + (at >= 2 * TERM).astype(jnp.int32)
        k = at - TERM * term
        dz = (k & 7) - row
        fits = (at < DEPTH) & (row < BLOCK) & (dz >= 0) & (dz < 3)
        return jnp.where(fits, (k >> 3) * 8 + dz, -1)

    code = (codes(lane), codes(lane + N))

    def fill(step, carry):
        space = step // 9
        entry = step % 9
        dy = entry // 3
        d = entry % 3
        rows = []
        for to in range(4):
            halves = [jnp.zeros((8, N), F32), jnp.zeros((8, N), F32)]
            for layer in range(2):
                dx = layer + 2 - to
                if dx < 0 or dx > 2:
                    continue
                for c in range(3):
                    for dz in range(3):
                        index = ((space * 27 + dx * 9 + dy * 3 + dz) * 3 + d) * 3 + c
                        value = table[pl.ds(index, 8, stride=0)]
                        for half in range(2 if c == 2 else 1):
                            hit = code[half] == (c * 2 + layer) * 8 + dz
                            halves[half] = jnp.where(hit, value, halves[half])
            parts = []
            for half, v in enumerate(halves):
                high = v.astype(BF16).astype(F32)
                parts.append(jnp.where(lane + half * N < 2 * TERM, high, v - high))
            rows.append(jnp.concatenate(parts, 1))
        start = pl.multiple_of(entry * 32, 32)
        out[space, pl.ds(start, 32)] = jnp.concatenate(rows, 0).astype(BF16)
        return carry

    lax.fori_loop(0, 36, fill, 0, unroll=3)


def correct(place, restricted, got, weights, out, first, second, w, sent):
    grp = place[0]
    blk = place[1]
    odd = blk % 2

    def dense(space, carry):
        for pair in range(PAIRS):
            starts = (2 * BLOCK * pair, 2 * BLOCK * pair + BLOCK)
            blocks = []
            for at in starts:
                inv = [got[space, layer * INV + at : layer * INV + at + 8] for layer in range(2)]
                blocks.append(jnp.concatenate([
                    restricted[space, c, layer, at : at + 8] * inv[layer]
                    for c in range(3) for layer in range(2)
                ], 0))
            fields = jnp.concatenate(blocks, 1)
            high = fields.astype(BF16)
            low = (fields - high.astype(F32)).astype(BF16)
            sums = jnp.dot(
                weights[space, :, 0:DEPTH],
                jnp.concatenate([high, low, high], 0),
                preferred_element_type=F32,
            )
            for half, at in enumerate(starts):
                lanes = slice(half * N, half * N + N)
                for d in range(3):
                    for to in range(4):
                        below, here, above = (
                            sums[row * 8 : row * 8 + 8, lanes]
                            for row in ((dy * 3 + d) * 4 + to for dy in range(3))
                        )
                        w[space, d, to, at : at + 8] = here + (
                            from_below(below) + from_above(above)
                        )
        return carry

    lax.fori_loop(0, 4, dense, 0, unroll=4)

    def clear(layers, rows):
        for space in range(4):
            for d in range(3):
                for layer in layers:
                    w[space, d, layer, rows] = jnp.zeros((rows.stop - rows.start, N), F32)

    @pl.when(grp == 0)
    def _():
        clear(range(4), slice(0, 1))

    @pl.when(grp == 3)
    def _():
        clear(range(4), slice(N + 1, N + 2))

    @pl.when(blk == 0)
    def _():
        clear((0,), slice(0, WROWS))

    @pl.when(blk == place[2])
    def _():
        clear((3,), slice(0, WROWS))

    for tile in range(N // 8):
        start = 8 * tile
        rows = slice(start, start + 8)

        def at(space, d, layer, shift):
            return w[space, d, layer, start + 1 + shift : start + 9 + shift]

        def along_x(shift):
            half = [0.5 * at(3, 0, layer, shift) for layer in range(4)]
            inner = [at(2, 0, layer, shift) + half[layer] for layer in range(4)]
            return [inner[0]] + [inner[i] + half[i - 1] for i in (1, 2, 3)] + [half[3]]

        def along_y(layer, shift):
            v = at(3, 1, layer, shift)
            return at(2, 1, layer, shift) + 0.5 * (v + from_below(v))

        def along_z(layer):
            return at(2, 2, layer, 0) + 0.5 * (at(3, 2, layer, 0) + at(3, 2, layer, -1))

        tx = along_x(0)
        tx_next = along_x(1)
        ty = [along_y(layer, 0) for layer in range(4)]
        tz = [along_z(layer) for layer in range(4)]
        y_sum = [0.25 * (at(1, 1, layer, 0) + at(1, 1, layer, 1)) for layer in range(4)]
        z_own = [at(1, 2, layer, 0) for layer in range(4)]
        z_sum = [0.25 * (v + from_above(v)) for v in z_own]
        xs, ys, zs = [], [], []
        for layer in range(4):
            x_sum = at(1, 0, layer, 0) + at(1, 0, layer, 1)
            xs.append(
                at(0, 0, layer, 0) + 0.25 * (x_sum + from_above(x_sum))
                + (ty[layer] - along_y(layer, 1)) - (tz[layer] - from_above(tz[layer]))
            )
        for layer in range(-1, 5):
            y = z = None
            if layer >= 0:
                y = tx_next[layer] - tx[layer]
                z = tx[layer] - from_above(tx[layer])
            if 0 <= layer < 4:
                y = y + (at(0, 1, layer, 0) + y_sum[layer] + tz[layer])
                z = z + (at(0, 2, layer, 0) + z_sum[layer] - ty[layer])
            if layer < 3:
                y_more = y_sum[layer + 1] - tz[layer + 1]
                z_more = z_sum[layer + 1] + ty[layer + 1]
                y = y_more if y is None else y + y_more
                z = z_more if z is None else z + z_more
            ys.append(y)
            zs.append(z)
        for layer in range(2):
            out[0, layer, rows] = xs[layer + 1]
            out[1, layer, rows] = ys[layer + 2]
            out[2, layer, rows] = zs[layer + 2]
        up = (xs[3], ys[4], zs[4], ys[5], zs[5])
        down = (xs[0], ys[1], zs[1], ys[0], zs[0])
        for slot in range(5):
            sent[1 - odd, slot, rows] = up[slot]
            sent[odd, slot, rows] = down[slot]
    first[...] = sent[0]
    second[...] = sent[1]


def combine(place, part, first, second, mask, out_hbm, total, out, sems):
    odd = place[1] % 2
    other = 1 - odd
    copies = []
    for comp in range(3):
        at_odd = part[comp, odd] + first[comp]
        at_other = part[comp, other] + second[comp]
        if comp > 0:
            at_odd += second[comp + 2]
            at_other += first[comp + 2]
        total[comp, odd] = at_odd
        total[comp, other] = at_other
        for layer in range(2):
            out[comp, layer] = total[comp, layer].T * mask[comp, layer].astype(F32)
        copies.append(pltpu.make_async_copy(out.at[comp], out_hbm.at[comp], sems.at[comp]))
        copies[-1].start()
    for copy in copies:
        copy.wait()


def correction(residual, face_mask, conductivity, stencil):
    blocks = lax.axis_size("blk")

    def swap(axis, message, begin):
        pairs = [(i, i + 1) for i in range(begin, lax.axis_size(axis) - 1, 2)]
        return lax.ppermute(message, axis, pairs + [(j, i) for i, j in pairs])

    def exchange(axis, first, second):
        return swap(axis, first, 1), swap(axis, second, 0)

    place = jnp.stack(
        [lax.axis_index("grp"), lax.axis_index("blk"), jnp.int32(blocks - 1)]
    ).astype(jnp.int32)

    at = [lax.broadcasted_iota(jnp.int32, stencil.shape, dim) for dim in range(4)]
    diagonal = at[2] == at[3]
    centre = jnp.where(diagonal[:, 13], stencil[:, 13], 0.0)
    step = OMEGA / centre.sum(2)
    twice = jnp.where(diagonal & (at[1] == 13), 2.0, 0.0)
    table = step[:, None, :, None] * (twice - stencil * step[:, None, None, :])
    table = jnp.broadcast_to(table.reshape(972, 1), (972, N))

    in_hbm = pl.BlockSpec(memory_space=pltpu.HBM)
    residual, mask, conductivity = (
        pltpu.with_memory_space_constraint(v, pltpu.HBM)
        for v in (residual, face_mask, conductivity)
    )
    own, first, second, chunks = call(
        mask_residual,
        [(3, 2, N, N), (2, N, N), (2, N, N), (4, 2 * INV, N)],
        [smem()] + [in_hbm] * 3,
        [
            pltpu.VMEM((1, 2, N, 4 * N), F32),
            pltpu.VMEM((3, 2, N, N), F32),
            pltpu.VMEM((3, 2, N, N), jnp.int32),
            pltpu.SemaphoreType.DMA((3,)),
        ],
    )(place, residual, mask, conductivity)
    x_first = swap("blk", first, 1)
    x_second = swap("blk", second, 0)
    got = lax.all_to_all(chunks, "grp", split_axis=0, concat_axis=0, tiled=True)
    (weights,) = call(band, [(4, 36 * 8, 2 * N)], [vmem()], dtype=BF16)(table)
    first, second = call(
        pack, [(PLANES, N), (PLANES, N)],
        [smem()] + [vmem()] * 3 + [pl.BlockSpec(memory_space=pl.ANY)],
        [pltpu.VMEM((2, PLANES, N), F32)],
    )(place, own, x_first, x_second, weights)
    z_first, z_second = exchange("grp", first, second)
    (restricted,) = call(
        restrict, [(4, 3, 2, HROWS, N)], [smem()] + [vmem()] * 5,
        [
            pltpu.VMEM((2, 3, MROWS, N), F32),
            pltpu.VMEM((2, 2, MROWS, N), F32),
            pltpu.VMEM((2, PLANES, N), F32),
        ],
    )(place, own, x_first, x_second, z_first, z_second)
    part, first, second = call(
        correct,
        [(3, 2, N, N), (5, N, N), (5, N, N)],
        [smem()] + [vmem()] * 3,
        [
            pltpu.VMEM((4, 3, 4, WROWS, N), F32),
            pltpu.VMEM((2, 5, N, N), F32),
        ],
    )(place, restricted, got, weights)
    first, second = exchange("blk", first, second)
    (out,) = call(
        combine, [(3, 2, N, N)], [smem()] + [vmem()] * 4,
        [
            pltpu.VMEM((3, 2, N, N), F32),
            pltpu.VMEM((3, 2, N, N), F32),
            pltpu.SemaphoreType.DMA((3,)),
        ],
        outs=in_hbm,
    )(place, part, first, second, face_mask)
    return out


def solution(mesh):
    return jax.shard_map(
        correction,
        mesh=mesh,
        in_specs=(
            P(None, "blk", None, "grp"),
            P(None, "blk", None, "grp"),
            P("grp", "blk", None, None),
            P(),
        ),
        out_specs=P(None, "blk", None, "grp"),
        check_vma=False,
    )
```

```python
import jax
import jax.numpy as jnp
from jax import lax
from jax.experimental import pallas as pl
from jax.experimental.pallas import tpu as pltpu
from jax.sharding import PartitionSpec as P

OMEGA = 0.8
F32 = jnp.float32
BF16 = jnp.bfloat16
N = 128
INV = 136
PLANES = 32
MROWS = 144
HROWS = 136
WROWS = 136
BLOCK = 6
PAIRS = 11
TERM = 48
DEPTH = 3 * TERM


def vmem():
    return pl.BlockSpec(memory_space=pltpu.VMEM)


def smem():
    return pl.BlockSpec(memory_space=pltpu.SMEM)


def call(kernel, out_shapes, in_specs, scratch=(), dtype=F32, outs=None):
    return pl.pallas_call(
        kernel,
        out_shape=[jax.ShapeDtypeStruct(shape, dtype) for shape in out_shapes],
        in_specs=in_specs,
        out_specs=outs or [vmem() for _ in out_shapes],
        scratch_shapes=list(scratch),
        compiler_params=pltpu.CompilerParams(vmem_limit_bytes=50 << 20),
    )


def from_below(v):
    lane = lax.broadcasted_iota(jnp.int32, v.shape, 1)
    return jnp.where(lane == 0, 0.0, pltpu.roll(v, 1, 1))


def from_above(v):
    lane = lax.broadcasted_iota(jnp.int32, v.shape, 1)
    return jnp.where(lane == N - 1, 0.0, pltpu.roll(v, N - 1, 1))


def mask_residual(
    place, res_hbm, mask_hbm, cond_hbm, own, first, second, chunks_hbm,
    chunks, cond, res, mask, sems,
):
    odd = place[1] % 2
    copies = [
        pltpu.make_async_copy(src, dst, sems.at[i])
        for i, (src, dst) in enumerate(((res_hbm, res), (mask_hbm, mask), (cond_hbm, cond)))
    ]
    for copy in copies:
        copy.start()
    copies[2].wait()
    invert(cond, chunks)
    leave = pltpu.make_async_copy(chunks, chunks_hbm, sems.at[3])
    leave.start()
    copies[0].wait()
    copies[1].wait()
    for comp in range(3):
        for layer in range(2):
            own[comp, layer] = (res[comp, layer] * mask[comp, layer].astype(F32)).T
    for slot in range(2):
        first[slot] = own[slot + 1, odd]
        second[slot] = own[slot + 1, 1 - odd]
    leave.wait()


def invert(cond, chunks):
    for layer in range(2):
        base = layer * INV
        chunks[0, base : base + 2] = jnp.zeros((2, N), F32)
        chunks[3, base + 130 : base + 132] = jnp.zeros((2, N), F32)
        for j in range(4):
            v = (1.0 / cond[0, layer, :, j * N : (j + 1) * N]).T
            chunks[j, base + 2 : base + 130] = v
            chunks[j, base + 132 : base + INV] = jnp.zeros((4, N), F32)
            if j < 3:
                chunks[j + 1, base : base + 2] = v[N - 2 : N]
            if j > 0:
                chunks[j - 1, base + 130 : base + 132] = v[0:2]


def plane_row(comp, layer):
    if layer in (0, 1):
        return (comp * 2 + layer) * 3
    return 18 + ((comp - 1) * 2 + max(layer, 0) // 2) * 3


def pack(place, own, x_first, x_second, weights, first, second, planes):
    z_odd = place[0] % 2
    odd = place[1] % 2

    def put(row, v):
        planes[0, row : row + 3] = v[0:3]
        planes[1, row : row + 3] = v[N - 3 : N]

    for comp in range(3):
        for layer in range(2):
            put(plane_row(comp, layer), own.at[comp, layer])
    for slot in range(2):
        low_row = plane_row(slot + 1, -1)
        for arrived, upper in ((x_first, odd), (x_second, 1 - odd)):
            row = low_row + 3 * upper
            v = arrived.at[slot]
            planes[0, pl.ds(row, 3)] = v[0:3]
            planes[1, pl.ds(row, 3)] = v[N - 3 : N]
    planes[:, 30:PLANES] = jnp.zeros((2, PLANES - 30, N), F32)
    first[...] = planes[z_odd]
    second[...] = planes[1 - z_odd]


def fill_masked(place, own, x_first, x_second, z_first, z_second, field, side, planes):
    z_odd = place[0] % 2
    odd = place[1] % 2
    planes[0] = z_first[...]
    planes[1] = z_second[...]
    for arrived, where in ((x_first, odd), (x_second, 1 - odd)):
        for slot in range(2):
            side[where, slot, 3 : 3 + N] = arrived[slot]

    def ends(ref, row):
        ref[0:3] = planes[z_odd, row : row + 3]
        ref[3 + N : 6 + N] = planes[1 - z_odd, row : row + 3]
        ref[6 + N : MROWS] = jnp.zeros((MROWS - N - 6, N), F32)

    for layer in range(2):
        for comp in range(3):
            field[layer, comp, 3 : 3 + N] = own[comp, layer]
            ends(field.at[layer, comp], plane_row(comp, layer))
    for where, layer in ((0, -1), (1, 2)):
        for slot in range(2):
            ends(side.at[where, slot], plane_row(slot + 1, layer))


def restrict_tile(field, side, place, start, rows):
    def at(layer, comp, shift):
        rows_at = slice(start + 1 + shift, start + 1 + shift + rows)
        if layer in (1, 2):
            return field[layer - 1, comp, rows_at]
        return side[layer // 3, comp - 1, rows_at]

    x0, xm, xp = (at(place, 0, s) for s in (0, -1, 1))
    y0, ym, yp = (at(place, 1, s) for s in (0, -1, 1))
    z0 = at(place, 2, 0)
    yl0, ylm, ylp = (at(place - 1, 1, s) for s in (0, -1, 1))
    zl0 = at(place - 1, 2, 0)
    yn0, ynm = (at(place + 1, 1, s) for s in (0, -1))
    zn0 = at(place + 1, 2, 0)
    xsum = x0 + xm
    zsum = z0 + zl0
    curl_x = z0 - from_below(z0) - y0 + ym
    curl_x_next = zn0 - from_below(zn0) - yn0 + ynm
    curl_y = x0 - xm - z0 + zl0
    curl_z = y0 - yl0 - x0 + from_below(x0)
    curl_z_next = yp - ylp - xp + from_below(xp)
    return (
        (x0, y0, z0),
        (
            0.25 * (xsum + from_below(xsum)),
            0.25 * (y0 + ym + (yl0 + ylm)),
            0.25 * (zsum + from_below(zsum)),
        ),
        (curl_x, curl_y, curl_z),
        (
            0.5 * (curl_x + curl_x_next),
            0.5 * (curl_y + from_above(curl_y)),
            0.5 * (curl_z + curl_z_next),
        ),
    )


def restrict(
    place, own, x_first, x_second, z_first, z_second, restricted, field, side, planes
):
    fill_masked(place, own, x_first, x_second, z_first, z_second, field, side, planes)
    for layer in range(2):
        for tile in range(HROWS // 8):
            start = 8 * tile
            spaces = restrict_tile(field, side, layer + 1, start, 8)
            for space in range(4):
                for comp in range(3):
                    restricted[space, comp, layer, start : start + 8] = spaces[space][comp]


def band(table, out):
    row = lax.broadcasted_iota(jnp.int32, (8, N), 0)
    lane = lax.broadcasted_iota(jnp.int32, (8, N), 1)

    def codes(at):
        term = (at >= TERM).astype(jnp.int32) + (at >= 2 * TERM).astype(jnp.int32)
        k = at - TERM * term
        dz = (k & 7) - row
        fits = (at < DEPTH) & (row < BLOCK) & (dz >= 0) & (dz < 3)
        return jnp.where(fits, (k >> 3) * 8 + dz, -1)

    code = (codes(lane), codes(lane + N))

    def fill(step, carry):
        space = step // 9
        entry = step % 9
        dy = entry // 3
        d = entry % 3
        rows = []
        for to in range(4):
            halves = [jnp.zeros((8, N), F32), jnp.zeros((8, N), F32)]
            for layer in range(2):
                dx = layer + 2 - to
                if dx < 0 or dx > 2:
                    continue
                for c in range(3):
                    for dz in range(3):
                        index = ((space * 27 + dx * 9 + dy * 3 + dz) * 3 + d) * 3 + c
                        value = table[pl.ds(index, 8, stride=0)]
                        for half in range(2 if c == 2 else 1):
                            hit = code[half] == (c * 2 + layer) * 8 + dz
                            halves[half] = jnp.where(hit, value, halves[half])
            parts = []
            for half, v in enumerate(halves):
                high = v.astype(BF16).astype(F32)
                parts.append(jnp.where(lane + half * N < 2 * TERM, high, v - high))
            rows.append(jnp.concatenate(parts, 1))
        start = pl.multiple_of(entry * 32, 32)
        out[space, pl.ds(start, 32)] = jnp.concatenate(rows, 0).astype(BF16)
        return carry

    lax.fori_loop(0, 36, fill, 0, unroll=3)


def correct(place, restricted, got, weights, out, first, second, w, sent):
    grp = place[0]
    blk = place[1]
    odd = blk % 2

    def dense(space, carry):
        for pair in range(PAIRS):
            starts = (2 * BLOCK * pair, 2 * BLOCK * pair + BLOCK)
            blocks = []
            for at in starts:
                inv = [got[space, layer * INV + at : layer * INV + at + 8] for layer in range(2)]
                blocks.append(jnp.concatenate([
                    restricted[space, c, layer, at : at + 8] * inv[layer]
                    for c in range(3) for layer in range(2)
                ], 0))
            fields = jnp.concatenate(blocks, 1)
            high = fields.astype(BF16)
            low = (fields - high.astype(F32)).astype(BF16)
            sums = jnp.dot(
                weights[space, :, 0:DEPTH],
                jnp.concatenate([high, low, high], 0),
                preferred_element_type=F32,
            )
            for half, at in enumerate(starts):
                lanes = slice(half * N, half * N + N)
                for d in range(3):
                    for to in range(4):
                        below, here, above = (
                            sums[row * 8 : row * 8 + 8, lanes]
                            for row in ((dy * 3 + d) * 4 + to for dy in range(3))
                        )
                        w[space, d, to, at : at + 8] = here + (
                            from_below(below) + from_above(above)
                        )
        return carry

    lax.fori_loop(0, 4, dense, 0, unroll=4)

    def clear(layers, rows):
        for space in range(4):
            for d in range(3):
                for layer in layers:
                    w[space, d, layer, rows] = jnp.zeros((rows.stop - rows.start, N), F32)

    @pl.when(grp == 0)
    def _():
        clear(range(4), slice(0, 1))

    @pl.when(grp == 3)
    def _():
        clear(range(4), slice(N + 1, N + 2))

    @pl.when(blk == 0)
    def _():
        clear((0,), slice(0, WROWS))

    @pl.when(blk == place[2])
    def _():
        clear((3,), slice(0, WROWS))

    for tile in range(N // 8):
        start = 8 * tile
        rows = slice(start, start + 8)

        def at(space, d, layer, shift):
            return w[space, d, layer, start + 1 + shift : start + 9 + shift]

        def along_x(shift):
            half = [0.5 * at(3, 0, layer, shift) for layer in range(4)]
            inner = [at(2, 0, layer, shift) + half[layer] for layer in range(4)]
            return [inner[0]] + [inner[i] + half[i - 1] for i in (1, 2, 3)] + [half[3]]

        def along_y(layer, shift):
            v = at(3, 1, layer, shift)
            return at(2, 1, layer, shift) + 0.5 * (v + from_below(v))

        def along_z(layer):
            return at(2, 2, layer, 0) + 0.5 * (at(3, 2, layer, 0) + at(3, 2, layer, -1))

        tx = along_x(0)
        tx_next = along_x(1)
        ty = [along_y(layer, 0) for layer in range(4)]
        tz = [along_z(layer) for layer in range(4)]
        y_sum = [0.25 * (at(1, 1, layer, 0) + at(1, 1, layer, 1)) for layer in range(4)]
        z_own = [at(1, 2, layer, 0) for layer in range(4)]
        z_sum = [0.25 * (v + from_above(v)) for v in z_own]
        xs, ys, zs = [], [], []
        for layer in range(4):
            x_sum = at(1, 0, layer, 0) + at(1, 0, layer, 1)
            xs.append(
                at(0, 0, layer, 0) + 0.25 * (x_sum + from_above(x_sum))
                + (ty[layer] - along_y(layer, 1)) - (tz[layer] - from_above(tz[layer]))
            )
        for layer in range(-1, 5):
            y = z = None
            if layer >= 0:
                y = tx_next[layer] - tx[layer]
                z = tx[layer] - from_above(tx[layer])
            if 0 <= layer < 4:
                y = y + (at(0, 1, layer, 0) + y_sum[layer] + tz[layer])
                z = z + (at(0, 2, layer, 0) + z_sum[layer] - ty[layer])
            if layer < 3:
                y_more = y_sum[layer + 1] - tz[layer + 1]
                z_more = z_sum[layer + 1] + ty[layer + 1]
                y = y_more if y is None else y + y_more
                z = z_more if z is None else z + z_more
            ys.append(y)
            zs.append(z)
        for layer in range(2):
            out[0, layer, rows] = xs[layer + 1]
            out[1, layer, rows] = ys[layer + 2]
            out[2, layer, rows] = zs[layer + 2]
        up = (xs[3], ys[4], zs[4], ys[5], zs[5])
        down = (xs[0], ys[1], zs[1], ys[0], zs[0])
        for slot in range(5):
            sent[1 - odd, slot, rows] = up[slot]
            sent[odd, slot, rows] = down[slot]
    first[...] = sent[0]
    second[...] = sent[1]


def combine(place, part, first, second, mask, out_hbm, total, out, sems):
    odd = place[1] % 2
    other = 1 - odd
    copies = []
    for comp in range(3):
        at_odd = part[comp, odd] + first[comp]
        at_other = part[comp, other] + second[comp]
        if comp > 0:
            at_odd += second[comp + 2]
            at_other += first[comp + 2]
        total[comp, odd] = at_odd
        total[comp, other] = at_other
        for layer in range(2):
            out[comp, layer] = total[comp, layer].T * mask[comp, layer].astype(F32)
        copies.append(pltpu.make_async_copy(out.at[comp], out_hbm.at[comp], sems.at[comp]))
        copies[-1].start()
    for copy in copies:
        copy.wait()


def correction(residual, face_mask, conductivity, stencil):
    blocks = lax.axis_size("blk")

    def swap(axis, message, begin):
        pairs = [(i, i + 1) for i in range(begin, lax.axis_size(axis) - 1, 2)]
        return lax.ppermute(message, axis, pairs + [(j, i) for i, j in pairs])

    def exchange(axis, first, second):
        return swap(axis, first, 1), swap(axis, second, 0)

    place = jnp.stack(
        [lax.axis_index("grp"), lax.axis_index("blk"), jnp.int32(blocks - 1)]
    ).astype(jnp.int32)

    at = [lax.broadcasted_iota(jnp.int32, stencil.shape, dim) for dim in range(4)]
    diagonal = at[2] == at[3]
    centre = jnp.where(diagonal[:, 13], stencil[:, 13], 0.0)
    step = OMEGA / centre.sum(2)
    twice = jnp.where(diagonal & (at[1] == 13), 2.0, 0.0)
    table = step[:, None, :, None] * (twice - stencil * step[:, None, None, :])
    table = jnp.broadcast_to(table.reshape(972, 1), (972, N))

    in_hbm = pl.BlockSpec(memory_space=pltpu.HBM)
    residual, mask, conductivity = (
        pltpu.with_memory_space_constraint(v, pltpu.HBM)
        for v in (residual, face_mask, conductivity)
    )
    own, first, second, chunks = call(
        mask_residual,
        [(3, 2, N, N), (2, N, N), (2, N, N), (4, 2 * INV, N)],
        [smem()] + [in_hbm] * 3,
        [
            pltpu.VMEM((4, 2 * INV, N), F32),
            pltpu.VMEM((1, 2, N, 4 * N), F32),
            pltpu.VMEM((3, 2, N, N), F32),
            pltpu.VMEM((3, 2, N, N), jnp.int32),
            pltpu.SemaphoreType.DMA((4,)),
        ],
        outs=[vmem()] * 3 + [in_hbm],
    )(place, residual, mask, conductivity)
    x_first = swap("blk", first, 1)
    x_second = swap("blk", second, 0)
    got = lax.all_to_all(chunks, "grp", split_axis=0, concat_axis=0, tiled=True)
    (weights,) = call(band, [(4, 36 * 8, 2 * N)], [vmem()], dtype=BF16)(table)
    first, second = call(
        pack, [(PLANES, N), (PLANES, N)],
        [smem()] + [vmem()] * 3 + [pl.BlockSpec(memory_space=pl.ANY)],
        [pltpu.VMEM((2, PLANES, N), F32)],
    )(place, own, x_first, x_second, weights)
    z_first, z_second = exchange("grp", first, second)
    (restricted,) = call(
        restrict, [(4, 3, 2, HROWS, N)], [smem()] + [vmem()] * 5,
        [
            pltpu.VMEM((2, 3, MROWS, N), F32),
            pltpu.VMEM((2, 2, MROWS, N), F32),
            pltpu.VMEM((2, PLANES, N), F32),
        ],
    )(place, own, x_first, x_second, z_first, z_second)
    part, first, second = call(
        correct,
        [(3, 2, N, N), (5, N, N), (5, N, N)],
        [smem()] + [vmem()] * 3,
        [
            pltpu.VMEM((4, 3, 4, WROWS, N), F32),
            pltpu.VMEM((2, 5, N, N), F32),
        ],
    )(place, restricted, got, weights)
    first, second = exchange("blk", first, second)
    (out,) = call(
        combine, [(3, 2, N, N)], [smem()] + [vmem()] * 4,
        [
            pltpu.VMEM((3, 2, N, N), F32),
            pltpu.VMEM((3, 2, N, N), F32),
            pltpu.SemaphoreType.DMA((3,)),
        ],
        outs=[in_hbm],
    )(place, part, first, second, face_mask)
    return out


def solution(mesh):
    return jax.shard_map(
        correction,
        mesh=mesh,
        in_specs=(
            P(None, "blk", None, "grp"),
            P(None, "blk", None, "grp"),
            P("grp", "blk", None, None),
            P(),
        ),
        out_specs=P(None, "blk", None, "grp"),
        check_vma=False,
    )
```

```python
import jax
import jax.numpy as jnp
from jax import lax
from jax.experimental import pallas as pl
from jax.experimental.pallas import tpu as pltpu
from jax.sharding import PartitionSpec as P

OMEGA = 0.8
F32 = jnp.float32
BF16 = jnp.bfloat16
N = 128
INV = 136
PLANES = 32
MROWS = 144
HROWS = 136
WROWS = 136
BLOCK = 6
PAIRS = 11
TERM = 48
DEPTH = 3 * TERM


def vmem():
    return pl.BlockSpec(memory_space=pltpu.VMEM)


def smem():
    return pl.BlockSpec(memory_space=pltpu.SMEM)


def call(kernel, out_shapes, in_specs, scratch=(), dtype=F32, outs=None):
    return pl.pallas_call(
        kernel,
        out_shape=[jax.ShapeDtypeStruct(shape, dtype) for shape in out_shapes],
        in_specs=in_specs,
        out_specs=outs or [vmem() for _ in out_shapes],
        scratch_shapes=list(scratch),
        compiler_params=pltpu.CompilerParams(vmem_limit_bytes=50 << 20),
    )


def from_below(v):
    lane = lax.broadcasted_iota(jnp.int32, v.shape, 1)
    return jnp.where(lane == 0, 0.0, pltpu.roll(v, 1, 1))


def from_above(v):
    lane = lax.broadcasted_iota(jnp.int32, v.shape, 1)
    return jnp.where(lane == N - 1, 0.0, pltpu.roll(v, N - 1, 1))


def mask_residual(
    place, res_hbm, mask_hbm, cond_hbm, own, first, second, chunks_hbm,
    chunks, cond, res, mask, sems,
):
    odd = place[1] % 2
    copies = [
        pltpu.make_async_copy(src, dst, sems.at[i])
        for i, (src, dst) in enumerate(((res_hbm, res), (mask_hbm, mask), (cond_hbm, cond)))
    ]
    for copy in copies:
        copy.start()
    copies[2].wait()
    invert(cond, chunks)
    leave = pltpu.make_async_copy(chunks, chunks_hbm, sems.at[3])
    leave.start()
    copies[0].wait()
    copies[1].wait()
    for comp in range(3):
        for layer in range(2):
            own[comp, layer] = (res[comp, layer] * mask[comp, layer].astype(F32)).T
    for slot in range(2):
        first[slot] = own[slot + 1, odd]
        second[slot] = own[slot + 1, 1 - odd]
    leave.wait()


def invert(cond, chunks):
    for layer in range(2):
        base = layer * INV
        chunks[0, base : base + 2] = jnp.zeros((2, N), F32)
        chunks[3, base + 130 : base + 132] = jnp.zeros((2, N), F32)
        for j in range(4):
            v = (1.0 / cond[0, layer, :, j * N : (j + 1) * N]).T
            chunks[j, base + 2 : base + 130] = v
            chunks[j, base + 132 : base + INV] = jnp.zeros((4, N), F32)
            if j < 3:
                chunks[j + 1, base : base + 2] = v[N - 2 : N]
            if j > 0:
                chunks[j - 1, base + 130 : base + 132] = v[0:2]


def plane_row(comp, layer):
    if layer in (0, 1):
        return (comp * 2 + layer) * 3
    return 18 + ((comp - 1) * 2 + max(layer, 0) // 2) * 3


def pack(place, own, x_first, x_second, weights, first, second, planes):
    z_odd = place[0] % 2
    odd = place[1] % 2

    def put(row, v):
        planes[0, row : row + 3] = v[0:3]
        planes[1, row : row + 3] = v[N - 3 : N]

    for comp in range(3):
        for layer in range(2):
            put(plane_row(comp, layer), own.at[comp, layer])
    for slot in range(2):
        low_row = plane_row(slot + 1, -1)
        for arrived, upper in ((x_first, odd), (x_second, 1 - odd)):
            row = low_row + 3 * upper
            v = arrived.at[slot]
            planes[0, pl.ds(row, 3)] = v[0:3]
            planes[1, pl.ds(row, 3)] = v[N - 3 : N]
    planes[:, 30:PLANES] = jnp.zeros((2, PLANES - 30, N), F32)
    first[...] = planes[z_odd]
    second[...] = planes[1 - z_odd]


def fill_masked(place, own, x_first, x_second, z_first, z_second, field, side, planes):
    z_odd = place[0] % 2
    odd = place[1] % 2
    planes[0] = z_first[...]
    planes[1] = z_second[...]
    for arrived, where in ((x_first, odd), (x_second, 1 - odd)):
        for slot in range(2):
            side[where, slot, 3 : 3 + N] = arrived[slot]

    def ends(ref, row):
        ref[0:3] = planes[z_odd, row : row + 3]
        ref[3 + N : 6 + N] = planes[1 - z_odd, row : row + 3]
        ref[6 + N : MROWS] = jnp.zeros((MROWS - N - 6, N), F32)

    for layer in range(2):
        for comp in range(3):
            field[layer, comp, 3 : 3 + N] = own[comp, layer]
            ends(field.at[layer, comp], plane_row(comp, layer))
    for where, layer in ((0, -1), (1, 2)):
        for slot in range(2):
            ends(side.at[where, slot], plane_row(slot + 1, layer))


def restrict_tile(field, side, place, start, rows):
    def at(layer, comp, shift):
        rows_at = slice(start + 1 + shift, start + 1 + shift + rows)
        if layer in (1, 2):
            return field[layer - 1, comp, rows_at]
        return side[layer // 3, comp - 1, rows_at]

    x0, xm, xp = (at(place, 0, s) for s in (0, -1, 1))
    y0, ym, yp = (at(place, 1, s) for s in (0, -1, 1))
    z0 = at(place, 2, 0)
    yl0, ylm, ylp = (at(place - 1, 1, s) for s in (0, -1, 1))
    zl0 = at(place - 1, 2, 0)
    yn0, ynm = (at(place + 1, 1, s) for s in (0, -1))
    zn0 = at(place + 1, 2, 0)
    xsum = x0 + xm
    zsum = z0 + zl0
    curl_x = z0 - from_below(z0) - y0 + ym
    curl_x_next = zn0 - from_below(zn0) - yn0 + ynm
    curl_y = x0 - xm - z0 + zl0
    curl_z = y0 - yl0 - x0 + from_below(x0)
    curl_z_next = yp - ylp - xp + from_below(xp)
    return (
        (x0, y0, z0),
        (
            0.25 * (xsum + from_below(xsum)),
            0.25 * (y0 + ym + (yl0 + ylm)),
            0.25 * (zsum + from_below(zsum)),
        ),
        (curl_x, curl_y, curl_z),
        (
            0.5 * (curl_x + curl_x_next),
            0.5 * (curl_y + from_above(curl_y)),
            0.5 * (curl_z + curl_z_next),
        ),
    )


def restrict(
    place, own, x_first, x_second, z_first, z_second, restricted, field, side, planes
):
    fill_masked(place, own, x_first, x_second, z_first, z_second, field, side, planes)
    for layer in range(2):
        for tile in range(HROWS // 8):
            start = 8 * tile
            spaces = restrict_tile(field, side, layer + 1, start, 8)
            for space in range(4):
                for comp in range(3):
                    restricted[space, comp, layer, start : start + 8] = spaces[space][comp]


def band(table, out):
    row = lax.broadcasted_iota(jnp.int32, (8, N), 0)
    lane = lax.broadcasted_iota(jnp.int32, (8, N), 1)

    def codes(at):
        term = (at >= TERM).astype(jnp.int32) + (at >= 2 * TERM).astype(jnp.int32)
        k = at - TERM * term
        dz = (k & 7) - row
        fits = (at < DEPTH) & (row < BLOCK) & (dz >= 0) & (dz < 3)
        return jnp.where(fits, (k >> 3) * 8 + dz, -1)

    code = (codes(lane), codes(lane + N))

    def fill(step, carry):
        space = step // 9
        entry = step % 9
        dy = entry // 3
        d = entry % 3
        rows = []
        for to in range(4):
            halves = [jnp.zeros((8, N), F32), jnp.zeros((8, N), F32)]
            for layer in range(2):
                dx = layer + 2 - to
                if dx < 0 or dx > 2:
                    continue
                for c in range(3):
                    for dz in range(3):
                        index = ((space * 27 + dx * 9 + dy * 3 + dz) * 3 + d) * 3 + c
                        value = table[pl.ds(index, 8, stride=0)]
                        for half in range(2 if c == 2 else 1):
                            hit = code[half] == (c * 2 + layer) * 8 + dz
                            halves[half] = jnp.where(hit, value, halves[half])
            parts = []
            for half, v in enumerate(halves):
                high = v.astype(BF16).astype(F32)
                parts.append(jnp.where(lane + half * N < 2 * TERM, high, v - high))
            rows.append(jnp.concatenate(parts, 1))
        start = pl.multiple_of(entry * 32, 32)
        out[space, pl.ds(start, 32)] = jnp.concatenate(rows, 0).astype(BF16)
        return carry

    lax.fori_loop(0, 36, fill, 0, unroll=3)


def correct(place, restricted, got, weights, out, first, second, w, sent):
    grp = place[0]
    blk = place[1]
    odd = blk % 2

    def dense(space, carry):
        for pair in range(PAIRS):
            starts = (2 * BLOCK * pair, 2 * BLOCK * pair + BLOCK)
            blocks = []
            for at in starts:
                inv = [got[space, layer * INV + at : layer * INV + at + 8] for layer in range(2)]
                blocks.append(jnp.concatenate([
                    restricted[space, c, layer, at : at + 8] * inv[layer]
                    for c in range(3) for layer in range(2)
                ], 0))
            fields = jnp.concatenate(blocks, 1)
            high = fields.astype(BF16)
            low = (fields - high.astype(F32)).astype(BF16)
            sums = jnp.dot(
                weights[space, :, 0:DEPTH],
                jnp.concatenate([high, low, high], 0),
                preferred_element_type=F32,
            )
            for half, at in enumerate(starts):
                lanes = slice(half * N, half * N + N)
                for d in range(3):
                    for to in range(4):
                        below, here, above = (
                            sums[row * 8 : row * 8 + 8, lanes]
                            for row in ((dy * 3 + d) * 4 + to for dy in range(3))
                        )
                        w[space, d, to, at : at + 8] = here + (
                            from_below(below) + from_above(above)
                        )
        return carry

    lax.fori_loop(0, 4, dense, 0, unroll=4)

    def clear(layers, rows):
        for space in range(4):
            for d in range(3):
                for layer in layers:
                    w[space, d, layer, rows] = jnp.zeros((rows.stop - rows.start, N), F32)

    @pl.when(grp == 0)
    def _():
        clear(range(4), slice(0, 1))

    @pl.when(grp == 3)
    def _():
        clear(range(4), slice(N + 1, N + 2))

    @pl.when(blk == 0)
    def _():
        clear((0,), slice(0, WROWS))

    @pl.when(blk == place[2])
    def _():
        clear((3,), slice(0, WROWS))

    for tile in range(N // 8):
        start = 8 * tile
        rows = slice(start, start + 8)

        def at(space, d, layer, shift):
            return w[space, d, layer, start + 1 + shift : start + 9 + shift]

        def along_x(shift):
            half = [0.5 * at(3, 0, layer, shift) for layer in range(4)]
            inner = [at(2, 0, layer, shift) + half[layer] for layer in range(4)]
            return [inner[0]] + [inner[i] + half[i - 1] for i in (1, 2, 3)] + [half[3]]

        def along_y(layer, shift):
            v = at(3, 1, layer, shift)
            return at(2, 1, layer, shift) + 0.5 * (v + from_below(v))

        def along_z(layer):
            return at(2, 2, layer, 0) + 0.5 * (at(3, 2, layer, 0) + at(3, 2, layer, -1))

        tx = along_x(0)
        tx_next = along_x(1)
        ty = [along_y(layer, 0) for layer in range(4)]
        tz = [along_z(layer) for layer in range(4)]
        y_sum = [0.25 * (at(1, 1, layer, 0) + at(1, 1, layer, 1)) for layer in range(4)]
        z_own = [at(1, 2, layer, 0) for layer in range(4)]
        z_sum = [0.25 * (v + from_above(v)) for v in z_own]
        xs, ys, zs = [], [], []
        for layer in range(4):
            x_sum = at(1, 0, layer, 0) + at(1, 0, layer, 1)
            xs.append(
                at(0, 0, layer, 0) + 0.25 * (x_sum + from_above(x_sum))
                + (ty[layer] - along_y(layer, 1)) - (tz[layer] - from_above(tz[layer]))
            )
        for layer in range(-1, 5):
            y = z = None
            if layer >= 0:
                y = tx_next[layer] - tx[layer]
                z = tx[layer] - from_above(tx[layer])
            if 0 <= layer < 4:
                y = y + (at(0, 1, layer, 0) + y_sum[layer] + tz[layer])
                z = z + (at(0, 2, layer, 0) + z_sum[layer] - ty[layer])
            if layer < 3:
                y_more = y_sum[layer + 1] - tz[layer + 1]
                z_more = z_sum[layer + 1] + ty[layer + 1]
                y = y_more if y is None else y + y_more
                z = z_more if z is None else z + z_more
            ys.append(y)
            zs.append(z)
        for layer in range(2):
            out[0, layer, rows] = xs[layer + 1]
            out[1, layer, rows] = ys[layer + 2]
            out[2, layer, rows] = zs[layer + 2]
        up = (xs[3], ys[4], zs[4], ys[5], zs[5])
        down = (xs[0], ys[1], zs[1], ys[0], zs[0])
        for slot in range(5):
            sent[1 - odd, slot, rows] = up[slot]
            sent[odd, slot, rows] = down[slot]
    first[...] = sent[0]
    second[...] = sent[1]


def combine(place, part, first, second, mask, out_hbm, total, out, sems):
    odd = place[1] % 2
    other = 1 - odd
    copies = []
    for comp in range(3):
        at_odd = part[comp, odd] + first[comp]
        at_other = part[comp, other] + second[comp]
        if comp > 0:
            at_odd += second[comp + 2]
            at_other += first[comp + 2]
        total[comp, odd] = at_odd
        total[comp, other] = at_other
        for layer in range(2):
            out[comp, layer] = total[comp, layer].T * mask[comp, layer].astype(F32)
            copies.append(pltpu.make_async_copy(
                out.at[comp, layer], out_hbm.at[comp, layer], sems.at[2 * comp + layer]
            ))
            copies[-1].start()
    for copy in copies:
        copy.wait()


def correction(residual, face_mask, conductivity, stencil):
    blocks = lax.axis_size("blk")

    def swap(axis, message, begin):
        pairs = [(i, i + 1) for i in range(begin, lax.axis_size(axis) - 1, 2)]
        return lax.ppermute(message, axis, pairs + [(j, i) for i, j in pairs])

    def exchange(axis, first, second):
        return swap(axis, first, 1), swap(axis, second, 0)

    place = jnp.stack(
        [lax.axis_index("grp"), lax.axis_index("blk"), jnp.int32(blocks - 1)]
    ).astype(jnp.int32)

    at = [lax.broadcasted_iota(jnp.int32, stencil.shape, dim) for dim in range(4)]
    diagonal = at[2] == at[3]
    centre = jnp.where(diagonal[:, 13], stencil[:, 13], 0.0)
    step = OMEGA / centre.sum(2)
    twice = jnp.where(diagonal & (at[1] == 13), 2.0, 0.0)
    table = step[:, None, :, None] * (twice - stencil * step[:, None, None, :])
    table = jnp.broadcast_to(table.reshape(972, 1), (972, N))

    in_hbm = pl.BlockSpec(memory_space=pltpu.HBM)
    residual, mask, conductivity = (
        pltpu.with_memory_space_constraint(v, pltpu.HBM)
        for v in (residual, face_mask, conductivity)
    )
    own, first, second, chunks = call(
        mask_residual,
        [(3, 2, N, N), (2, N, N), (2, N, N), (4, 2 * INV, N)],
        [smem()] + [in_hbm] * 3,
        [
            pltpu.VMEM((4, 2 * INV, N), F32),
            pltpu.VMEM((1, 2, N, 4 * N), F32),
            pltpu.VMEM((3, 2, N, N), F32),
            pltpu.VMEM((3, 2, N, N), jnp.int32),
            pltpu.SemaphoreType.DMA((4,)),
        ],
        outs=[vmem()] * 3 + [in_hbm],
    )(place, residual, mask, conductivity)
    x_first = swap("blk", first, 1)
    x_second = swap("blk", second, 0)
    got = lax.all_to_all(chunks, "grp", split_axis=0, concat_axis=0, tiled=True)
    (weights,) = call(band, [(4, 36 * 8, 2 * N)], [vmem()], dtype=BF16)(table)
    first, second = call(
        pack, [(PLANES, N), (PLANES, N)],
        [smem()] + [vmem()] * 3 + [pl.BlockSpec(memory_space=pl.ANY)],
        [pltpu.VMEM((2, PLANES, N), F32)],
    )(place, own, x_first, x_second, weights)
    z_first, z_second = exchange("grp", first, second)
    (restricted,) = call(
        restrict, [(4, 3, 2, HROWS, N)], [smem()] + [vmem()] * 5,
        [
            pltpu.VMEM((2, 3, MROWS, N), F32),
            pltpu.VMEM((2, 2, MROWS, N), F32),
            pltpu.VMEM((2, PLANES, N), F32),
        ],
    )(place, own, x_first, x_second, z_first, z_second)
    part, first, second = call(
        correct,
        [(3, 2, N, N), (5, N, N), (5, N, N)],
        [smem()] + [vmem()] * 3,
        [
            pltpu.VMEM((4, 3, 4, WROWS, N), F32),
            pltpu.VMEM((2, 5, N, N), F32),
        ],
    )(place, restricted, got, weights)
    first, second = exchange("blk", first, second)
    (out,) = call(
        combine, [(3, 2, N, N)], [smem()] + [vmem()] * 4,
        [
            pltpu.VMEM((3, 2, N, N), F32),
            pltpu.VMEM((3, 2, N, N), F32),
            pltpu.SemaphoreType.DMA((6,)),
        ],
        outs=[in_hbm],
    )(place, part, first, second, face_mask)
    return out


def solution(mesh):
    return jax.shard_map(
        correction,
        mesh=mesh,
        in_specs=(
            P(None, "blk", None, "grp"),
            P(None, "blk", None, "grp"),
            P("grp", "blk", None, None),
            P(),
        ),
        out_specs=P(None, "blk", None, "grp"),
        check_vma=False,
    )
```
